128 devices in a mesh: expert: 4 (over z), shard: 32 (over y, x, core).
Axes of the slice: x: 4, y: 4, z: 4, core: 2. Of those that a mesh axis runs over, the one named last changes fastest.
Arguments:
- master_gate: float32 [64, 2048, 1408], P('expert', 'shard'), may hold values from -0.25 to 0.25
- master_up: float32 [64, 2048, 1408], P('expert', 'shard'), may hold values from -0.25 to 0.25
- router_weight: float32 [2048, 64], P('shard', 'expert'), may hold values from -0.125 to 0.125
- router_gain: float32 [2048], P('shard'), may hold values from 0.25 to 1.75
Outputs:
- final_gate: bfloat16 [64, 2048, 1408], P('expert', None, 'shard')
- final_up: bfloat16 [64, 2048, 1408], P('expert', None, 'shard')
- scale_gate: float32 [64, 1408], P('expert', 'shard')
- scale_up: float32 [64, 1408], P('expert', 'shard')
- serve_router: bfloat16 [2048, 64], replicated
The draws below stay inside these ranges and needn't reach their ends.
All inputs are finite; a program needn't handle non-finite values.
Results may differ from the reference program's by a relative error of at most 0.001.
Values may be sent and summed in bfloat16 or wider, within the bound.
A program may use at most 128 MiB of HBM per device.

```python
import jax
import jax.numpy as jnp
from jax import lax

EXPERTS = 64
D_MODEL = 2048
D_EXPERT = 1408


def strengthened(entries, stream_key, source, target, blocks, factor):
    def block_of(position):
        return (jnp.arange(entries.shape[position]) // (entries.shape[position] // blocks)).reshape((-1,) + (1,) * (entries.ndim - 1 - position))

    one_side = jax.random.permutation(stream_key, blocks)[block_of(target)]
    second = (block_of(target) + blocks // 2) % blocks
    return jnp.where((block_of(source) == one_side) | (block_of(source) == second), factor * entries, entries)


def block_levels(key, dims, pieces, least, top_value):
    def one(position, shards_of):
        heights = jax.random.uniform(jax.random.fold_in(jax.random.fold_in(key, 6), position), (shards_of,), jnp.float32, least / len(pieces), top_value / len(pieces))
        return jnp.repeat(jnp.exp(heights), dims[position] // shards_of).reshape((-1,) + (1,) * (len(dims) - position - 1))

    level = one(*pieces[0])
    for cut in pieces[1:]:
        level = level * one(*cut)
    return level


def bell_draw(own_key, extent, deviation, limit, pieces=(), held_as=jnp.bfloat16):
    result = deviation * jax.random.normal(own_key, extent, jnp.float32)
    if pieces:
        result = result * block_levels(own_key, extent, pieces, -0.22, 0.18)
    return jnp.clip(result, -limit, limit).astype(held_as)


def gaussian_with(rng, shape, width, bound, pieces, heavy, kind=jnp.bfloat16):
    entries = width * jax.random.normal(rng, shape, jnp.float32)
    if pieces:
        entries = entries * block_levels(rng, shape, pieces, -0.22, 0.18)
    return jnp.clip(strengthened(entries, jax.random.fold_in(rng, 3), *heavy), -bound, bound).astype(kind)


def setup_inputs(seed: int = 0) -> dict:
    seeds = jax.random.split(jax.random.key(seed), 5)
    master_gate = gaussian_with(seeds[0], (EXPERTS, D_MODEL, D_EXPERT), D_MODEL ** -0.5, 0.25, ((0, 4), (1, 32)), (1, 2, 32, 2.75), jnp.float32)
    master_up = gaussian_with(seeds[1], (EXPERTS, D_MODEL, D_EXPERT), D_MODEL ** -0.5, 0.25, ((0, 4), (1, 32)), (1, 2, 32, 2.75), jnp.float32)
    router_weight = bell_draw(seeds[2], (D_MODEL, EXPERTS), D_MODEL ** -0.5, 0.125, ((0, 32), (1, 4)), jnp.float32)
    router_gain = jnp.clip(1.0 + 0.15 * jax.random.normal(seeds[3], (D_MODEL,), jnp.float32), 0.25, 1.75)
    return dict(master_gate=master_gate, master_up=master_up, router_weight=router_weight, router_gain=router_gain)


def reference(master_gate, master_up, router_weight, router_gain):
    scale_gate = jnp.sqrt(lax.optimization_barrier(jnp.sum(master_gate * master_gate, axis=1)))
    final_gate = (master_gate / jnp.expand_dims(scale_gate, 1)).astype(jnp.bfloat16)
    scale_up = jnp.sqrt(lax.optimization_barrier(jnp.sum(master_up * master_up, axis=1)))
    final_up = (master_up / jnp.expand_dims(scale_up, 1)).astype(jnp.bfloat16)
    serve_router = (router_weight * router_gain[:, None]).astype(jnp.bfloat16)
    return (final_gate, final_up, scale_gate, scale_up, serve_router)
```

```python
import jax
import jax.numpy as jnp
from jax import lax
from jax.experimental import pallas as pl
from jax.experimental.pallas import tpu as pltpu
from jax.sharding import PartitionSpec as P

MESH = pl.DeviceIdType.MESH
LANES = 128
SPAN = 250.0
FLOOR = 124.0
MIX, START = 11, 16


def encoded(x, partial):
    rate = jnp.where(partial > 0, SPAN * lax.rsqrt(partial), 0.0)
    code = jnp.exp2(jnp.abs(x) * rate - FLOOR)
    return jnp.where(x < 0, -code, code)


def make_kernel(experts, rows, width, group, cols, n_y, n_x, n_z):
    n = n_y * n_x * 2
    half = experts // 2
    blocks = width // LANES
    pieces = 2
    part = cols // pieces
    prow = part * half
    n_msg = 2 * (pieces + 1)

    def kernel(gate, up, router, gain, og, ou, osg, osu, orr,
               xg, xu, stage, code, got, sums, msg, inbox, factor, zbuf, zgot,
               in_sem, own_sem, send_sem, recv_sem, zsend, zrecv):
        me = lax.axis_index("shard")
        plane = lax.axis_index("expert")
        my_y, my_x, my_k = me // (2 * n_x), (me // 2) % n_x, me % 2

        def load(h, t):
            src, dst = ((gate, xg), (up, xu))[t]
            return pltpu.make_async_copy(
                src.at[pl.ds(h * half, half)], dst.at[pl.ds(h * half, half)], in_sem.at[h, t]
            )

        for h in range(2):
            for t in range(2):
                load(h, t).start()

        def greet(d, _):
            pl.semaphore_signal(
                barrier, 1, device_id={"shard": lax.rem(me + d, n)}, device_id_type=MESH
            )
            return _

        barrier = pltpu.get_barrier_semaphore()
        lax.fori_loop(1, n, greet, 0)
        for d in range(1, n_z):
            pl.semaphore_signal(
                barrier, 1, device_id={"expert": lax.rem(plane + d, n_z)}, device_id_type=MESH
            )

        lane = lax.broadcasted_iota(jnp.int32, (half, LANES), 1)
        left = lane < LANES // 2
        folded = router[...] * gain[...]
        folded = jnp.concatenate([folded[:half], folded[half:]], axis=1)

        def produce(h):
            def block(b, _):
                at = pl.ds(pl.multiple_of(b * LANES, LANES), LANES)
                for e in range(half):
                    g = xg[h * half + e, :, at]
                    u = xu[h * half + e, :, at]
                    pg = jnp.sum(g * g, axis=0, keepdims=True)
                    pu = jnp.sum(u * u, axis=0, keepdims=True)
                    sums[h, 0, pl.ds(e, 1), at] = pg
                    sums[h, 1, pl.ds(e, 1), at] = pu
                    both = jnp.concatenate([encoded(g, pg), encoded(u, pu)], axis=0)
                    stage[pl.ds(e, LANES, stride=half), :] = both.T
                code[h, pl.ds(pl.multiple_of(b * LANES * half, LANES * half), LANES * half), :] = stage[...].astype(jnp.bfloat16)
                return _

            lax.fori_loop(0, blocks, block, 0)

            def message(q, _):
                first = q * cols
                lo = pl.multiple_of(first // LANES * LANES, LANES)
                s = lax.rem(first, LANES)
                quads = []
                for t, shift in ((0, lax.rem(LANES - s, LANES)), (1, lax.rem(LANES + LANES // 2 - s, LANES))):
                    a = sums[h, t, :, pl.ds(lo, LANES)]
                    b = sums[h, t, :, pl.ds(lo + LANES, LANES)]
                    a, b = pltpu.roll(a, shift, axis=1), pltpu.roll(b, shift, axis=1)
                    quads.append(jnp.where(lane - t * (LANES // 2) + s < LANES, a, b))
                msg[q, pl.ds(2 * h * half, half), :] = jnp.where(left, quads[0], quads[1])
                if h == 0:
                    msg[q, pl.ds(half, half), :] = folded
                return _

            lax.fori_loop(0, n, message, 0)

        def peer(d):
            y = lax.rem(my_y + d // (2 * n_x), n_y)
            x = lax.rem(my_x + (d // 2) % n_x, n_x)
            k = lax.rem(my_k + d % 2, 2)
            return (y * n_x + x) * 2 + k

        def slices(m):
            h, c = m // (pieces + 1), m % (pieces + 1)
            return h, c

        def remote(m, q, s):
            h, c = slices(m)
            if c == 0:
                rng = pl.ds(0, 2 * half) if h == 0 else pl.ds(2 * half, half)
                src, dst = msg.at[q, rng], inbox.at[s, rng]
            else:
                src = code.at[h, pl.ds(pl.multiple_of(q * cols * half + (c - 1) * prow, 2 * half), prow)]
                dst = got.at[h, s, pl.ds((c - 1) * prow, prow)]
            return pltpu.make_async_remote_copy(
                src, dst, send_sem.at[m, q], recv_sem.at[m, s],
                device_id={"shard": q}, device_id_type=MESH,
            )

        def each_peer(act):
            def one(i, _):
                act(peer(lax.rem(i * MIX + START, n)))
                return _

            skip = (-START * pow(MIX, -1, n)) % n
            lax.fori_loop(0, skip, one, 0)
            lax.fori_loop(skip + 1, n, one, 0)

        def own(h):
            return pltpu.make_async_copy(
                code.at[h, pl.ds(pl.multiple_of(me * cols * half, 2 * half), cols * half)],
                got.at[h, me], own_sem.at[h],
            )

        for h in range(2):
            for t in range(2):
                load(h, t).wait()
            produce(h)
            if h == 0:
                pl.semaphore_wait(barrier, n - 1 + n_z - 1)
            for c in range(pieces + 1):
                each_peer(lambda q: remote(h * (pieces + 1) + c, q, me).start())
            own(h).start()
            inbox[me, pl.ds(2 * h * half, half), :] = msg[me, pl.ds(2 * h * half, half), :]
            if h == 0:
                inbox[me, pl.ds(half, half), :] = folded

        def arrived(m):
            each_peer(lambda q: remote(m, me, q).wait_recv())

        arrived(0)

        def join(c, _):
            a, b = inbox[2 * c, pl.ds(half, half), :], inbox[2 * c + 1, pl.ds(half, half), :]
            low = jnp.where(left, a, pltpu.roll(b, LANES // 2, axis=1))
            high = jnp.where(left, pltpu.roll(a, LANES // 2, axis=1), b)
            zbuf[:, pl.ds(pl.multiple_of(c * LANES, LANES), LANES)] = jnp.concatenate([low, high], axis=0).astype(jnp.bfloat16)
            return _

        lax.fori_loop(0, n // 2, join, 0)

        def across(d):
            z = lax.rem(plane + d, n_z)
            return pltpu.make_async_remote_copy(
                zbuf, zgot.at[plane], zsend.at[d], zrecv.at[plane],
                device_id={"expert": z}, device_id_type=MESH,
            )

        def from_across(d):
            z = lax.rem(plane + d, n_z)
            return pltpu.make_async_remote_copy(
                zbuf, zgot.at[z], zsend.at[d], zrecv.at[z],
                device_id={"expert": z}, device_id_type=MESH,
            )

        for d in range(1, n_z):
            across(d).start()
        orr[pl.ds(pl.multiple_of(plane * experts, experts), experts), :] = zbuf[...]

        def factors(h):
            rng = pl.ds(2 * h * half, half)
            total = lax.fori_loop(0, n, lambda s, t: t + inbox[s, rng, :], jnp.zeros((half, LANES), jnp.float32))
            scale = jnp.sqrt(total)
            osg[pl.ds(h * half, half), :] = scale[:, :cols]
            osu[pl.ds(h * half, half), :] = pltpu.roll(scale, LANES // 2, axis=1)[:, :cols]
            share = 1.0 / (SPAN * scale)

            def one(s, _):
                factor[s] = jnp.sqrt(inbox[s, rng, :]) * share
                return _

            lax.fori_loop(0, n, one, 0)

        pick = jnp.where(left, 0, LANES // 2)

        def decode(h, c):
            m = h * (pieces + 1) + 1 + c

            def chip(i, _):
                dc = lax.rem(START // 2 + MIX * i, n // 2)
                y = lax.rem(my_y - dc // n_x + n_y, n_y)
                x = lax.rem(my_x - dc % n_x + n_x, n_x)
                at = y * n_x + x
                for k in range(2):
                    s = 2 * at + k

                    @pl.when(s != me)
                    def arrival():
                        remote(m, me, s).wait_recv()

                fa, fb = factor[2 * at], factor[2 * at + 1]
                lanes_out = pl.ds(pl.multiple_of(at * LANES, LANES), LANES)
                for p in range(part // 2):
                    base = c * prow + p * 2 * half
                    pair = []
                    for s, f in ((2 * at, fa), (2 * at + 1, fb)):
                        v = got[h, s, pl.ds(base, 2 * half), :].astype(jnp.float32)
                        j = c * part + 2 * p
                        mul = jnp.concatenate(
                            [jnp.take_along_axis(f, pick + j, axis=1), jnp.take_along_axis(f, pick + (j + 1), axis=1)], axis=0
                        )
                        w = (jnp.log2(jnp.abs(v)) + FLOOR) * mul
                        pair.append(jnp.where(v < 0, -w, w))
                    a, b = pair
                    l2 = jnp.concatenate([left, left], axis=0)
                    turned = pltpu.roll(jnp.where(l2, b, a), LANES // 2, axis=1)
                    fg = jnp.where(l2, a, turned).astype(jnp.bfloat16)
                    fu = jnp.where(l2, turned, b).astype(jnp.bfloat16)
                    for r in range(2):
                        og[j + r, pl.ds(h * half, half), lanes_out] = fg[r * half:(r + 1) * half]
                        ou[j + r, pl.ds(h * half, half), lanes_out] = fu[r * half:(r + 1) * half]
                return _

            lax.fori_loop(0, n // 2, chip, 0)

        for h in range(2):
            if h == 1:
                arrived(pieces + 1)
            factors(h)
            own(h).wait()
            for c in range(pieces):
                decode(h, c)

        for d in range(1, n_z):
            across(d).wait_send()
            from_across(d).wait_recv()
            z = lax.rem(plane + d, n_z)
            orr[pl.ds(pl.multiple_of(z * experts, experts), experts), :] = zgot[z]
        for m in range(n_msg):
            each_peer(lambda q: remote(m, q, me).wait_send())

    return kernel


def solution(mesh):
    n_z, n = mesh.shape["expert"], mesh.shape["shard"]
    n_y = n_x = 4

    def local(master_gate, master_up, router_weight, router_gain):
        experts, rows, width = master_gate.shape
        cols = width // n
        depth = rows * n
        half = experts // 2
        f32, bf16 = jnp.float32, jnp.bfloat16
        vmem = pl.BlockSpec(memory_space=pltpu.VMEM)
        hbm = pl.BlockSpec(memory_space=pl.ANY)
        dma = pltpu.SemaphoreType.DMA
        og, ou, osg, osu, orr = pl.pallas_call(
            make_kernel(experts, rows, width, None, cols, n_y, n_x, n_z),
            out_shape=(
                jax.ShapeDtypeStruct((cols, experts, depth), bf16),
                jax.ShapeDtypeStruct((cols, experts, depth), bf16),
                jax.ShapeDtypeStruct((experts, cols), f32),
                jax.ShapeDtypeStruct((experts, cols), f32),
                jax.ShapeDtypeStruct((experts * n_z, depth), bf16),
            ),
            in_specs=[hbm, hbm, vmem, vmem],
            out_specs=(vmem,) * 5,
            scratch_shapes=[
                pltpu.VMEM((experts, rows, width), f32),
                pltpu.VMEM((experts, rows, width), f32),
                pltpu.VMEM((LANES * half, LANES), f32),
                pltpu.VMEM((2, width * half, LANES), bf16),
                pltpu.VMEM((2, n, cols * half, LANES), bf16),
                pltpu.VMEM((2, 2, half, width + LANES), f32),
                pltpu.VMEM((n, 3 * half, LANES), f32),
                pltpu.VMEM((n, 3 * half, LANES), f32),
                pltpu.VMEM((n, half, LANES), f32),
                pltpu.VMEM((experts, depth), bf16),
                pltpu.VMEM((n_z, experts, depth), bf16),
                dma((2, 2)), dma((2,)), dma((6, n)), dma((6, n)), dma((n_z,)), dma((n_z,)),
            ],
            compiler_params=pltpu.CompilerParams(
                collective_id=0, has_side_effects=True, vmem_limit_bytes=48 * 2**20
            ),
        )(master_gate, master_up, router_weight.T, router_gain[None, :])
        return (
            og.transpose(1, 2, 0),
            ou.transpose(1, 2, 0),
            osg,
            osu,
            orr.T,
        )

    in_specs = (P("expert", "shard", None), P("expert", "shard", None), P("shard", "expert"), P("shard"))
    out_specs = (P("expert", None, "shard"), P("expert", None, "shard"), P("expert", "shard"), P("expert", "shard"), P())
    return jax.shard_map(local, mesh=mesh, in_specs=in_specs, out_specs=out_specs, check_vma=False)
```

```python
import jax
import jax.numpy as jnp
from jax import lax
from jax.experimental import pallas as pl
from jax.experimental.pallas import tpu as pltpu
from jax.sharding import PartitionSpec as P

MESH = pl.DeviceIdType.MESH
LANES = 128
SUBS = 8
SPAN = 250.0
FLOOR = 124.0
MIX, START = 11, 16
QUARTERS = 4


def encoded(x, partial):
    rate = jnp.where(partial > 0, SPAN * lax.rsqrt(partial), 0.0)
    code = jnp.exp2(jnp.abs(x) * rate - FLOOR)
    return jnp.where(x < 0, -code, code)


def make_kernel(experts, rows, width, cols, n_y, n_x, n_z):
    n = n_y * n_x * 2
    chips = n // 2
    few = experts // QUARTERS
    blocks = width // LANES
    piece = cols * few
    half_lane = LANES // 2

    def kernel(gate, up, router, gain, og, ou, osg, osu, orr,
               xg, xu, stage, code, got, sums, msg, inbox, factor, xr, xgain, rtile, rin, zbuf, zgot,
               in_sem, small_sem, own_sem, send_sem, recv_sem, sums_send, sums_recv, rsend, rrecv, pair_sem, zsend, zrecv):
        me = lax.axis_index("shard")
        plane = lax.axis_index("expert")
        my_chip, my_k = me // 2, me % 2
        my_y, my_x = my_chip // n_x, my_chip % n_x

        def load(a, t):
            src, dst = ((gate, xg), (up, xu))[t]
            return pltpu.make_async_copy(src.at[pl.ds(a * few, few)], dst.at[pl.ds(a * few, few)], in_sem.at[a, t])

        small = [pltpu.make_async_copy(router, xr, small_sem.at[0]), pltpu.make_async_copy(gain, xgain, small_sem.at[1])]
        for t in range(2):
            load(0, t).start()
        for c in small:
            c.start()
        barrier = pltpu.get_barrier_semaphore()
        for d in range(1, n_z):
            pl.semaphore_signal(barrier, 1, device_id={"expert": lax.rem(plane + d, n_z)}, device_id_type=MESH)

        def chip_at(d):
            y = lax.rem(my_y + d // (2 * n_x), n_y)
            x = lax.rem(my_x + (d // 2) % n_x, n_x)
            return y * n_x + x

        order = [d for d in ((i * MIX + START) % n for i in range(n)) if d]
        peers = [chip_at(d) * 2 + lax.rem(my_k + d % 2, 2) for d in order]
        for q in peers:
            pl.semaphore_signal(barrier, 1, device_id={"shard": q}, device_id_type=MESH)
        for a in range(1, QUARTERS):
            for t in range(2):
                load(a, t).start()

        row = lax.broadcasted_iota(jnp.int32, (SUBS, LANES), 0)
        lane = lax.broadcasted_iota(jnp.int32, (SUBS, LANES), 1)
        left = lane < half_lane
        upper = row < few

        def across_lanes(v):
            return pltpu.roll(v, half_lane, axis=1)

        def produce(a):
            h, e0 = a // 2, (a % 2) * few

            def block(b, z):
                at = pl.ds(pl.multiple_of(b * LANES, LANES), LANES)
                for e in range(few):
                    g = xg[a * few + e, :, at]
                    u = xu[a * few + e, :, at]
                    pg = jnp.sum(g * g, axis=0, keepdims=True)
                    pu = jnp.sum(u * u, axis=0, keepdims=True)
                    sums[h, 0, pl.ds(e0 + e, 1), at] = pg
                    sums[h, 1, pl.ds(e0 + e, 1), at] = pu
                    both = jnp.concatenate([encoded(g, pg), encoded(u, pu)], axis=0)
                    stage[pl.ds(e, LANES, stride=few), :] = both.T
                size = LANES * few
                code[a, pl.ds(pl.multiple_of(b * size, size), size), :] = stage[...].astype(jnp.bfloat16)
                return z

            lax.fori_loop(0, blocks, block, 0)

        def message(h):
            def one(q, z):
                first = q * cols
                lo = pl.multiple_of(first // LANES * LANES, LANES)
                s = lax.rem(first, LANES)
                sides = []
                for t, shift in ((0, lax.rem(LANES - s, LANES)), (1, lax.rem(LANES + half_lane - s, LANES))):
                    a = pltpu.roll(sums[h, t, :, pl.ds(lo, LANES)], shift, axis=1)
                    b = pltpu.roll(sums[h, t, :, pl.ds(lo + LANES, LANES)], shift, axis=1)
                    sides.append(jnp.where(lane - t * half_lane + s < LANES, a, b))
                msg[h, q] = jnp.where(left, sides[0], sides[1])
                return z

            lax.fori_loop(0, n, one, 0)
            inbox[h, me] = msg[h, me]

        def piece_to(a, q):
            return pltpu.make_async_remote_copy(
                code.at[a, pl.ds(pl.multiple_of(q * piece, 16), piece)], got.at[a, me],
                send_sem.at[a], recv_sem.at[a, me], device_id={"shard": q}, device_id_type=MESH,
            )

        def piece_from(a, s):
            return pltpu.make_async_remote_copy(
                got.at[a, s], got.at[a, s], send_sem.at[a], recv_sem.at[a, s], device_id={"shard": s}, device_id_type=MESH,
            )

        def all_pieces(a):
            ref = code.at[a, pl.ds(0, (n - 1) * piece)]
            return pltpu.make_async_remote_copy(
                ref, ref, send_sem.at[a], recv_sem.at[a, 0], device_id={"shard": me}, device_id_type=MESH
            )

        def sums_to(h, q):
            return pltpu.make_async_remote_copy(
                msg.at[h, q], inbox.at[h, me], sums_send.at[h], sums_recv.at[h], device_id={"shard": q}, device_id_type=MESH
            )

        def all_sums(h):
            src, dst = msg.at[h, pl.ds(0, n - 1)], inbox.at[h, pl.ds(0, n - 1)]
            return pltpu.make_async_remote_copy(
                src, dst, sums_send.at[h], sums_recv.at[h], device_id={"shard": me}, device_id_type=MESH
            )

        def own(a):
            return pltpu.make_async_copy(
                code.at[a, pl.ds(pl.multiple_of(me * piece, 16), piece)], got.at[a, me], own_sem.at[a]
            )

        def tile_to(q):
            return pltpu.make_async_remote_copy(
                rtile, rin.at[my_k, my_chip], rsend, rrecv, device_id={"shard": q}, device_id_type=MESH
            )

        def all_tiles():
            ref = rin.at[0, pl.ds(0, chips - 1)]
            return pltpu.make_async_remote_copy(ref, ref, rsend, rrecv, device_id={"shard": me}, device_id_type=MESH)

        def to_partner(k):
            return pltpu.make_async_remote_copy(
                rin.at[k], rin.at[k], pair_sem.at[0], pair_sem.at[1],
                device_id={"shard": my_chip * 2 + 1 - my_k}, device_id_type=MESH,
            )

        for a in range(QUARTERS):
            for t in range(2):
                load(a, t).wait()
            produce(a)
            if a == 0:
                for c in small:
                    c.wait()
                folded = xr[...] * xgain[...]
                rtile[...] = jnp.concatenate([folded[:SUBS], folded[SUBS:]], axis=1).astype(jnp.bfloat16)
                rin[my_k, my_chip] = rtile[...]
                pl.semaphore_wait(barrier, n - 1 + n_z - 1)
            if a % 2:
                message(a // 2)
                for q in peers:
                    sums_to(a // 2, q).start()
            for q in peers:
                piece_to(a, q).start()
            own(a).start()
            if a == 0:
                for d, q in zip(order, peers):
                    if d % 2 == 0:
                        tile_to(q).start()

        all_tiles().wait_recv()
        to_partner(my_k).start()
        to_partner(1 - my_k).wait_recv()

        def join(c, z):
            a, b = rin[0, c].astype(jnp.float32), rin[1, c].astype(jnp.float32)
            low = jnp.where(left, a, across_lanes(b))
            high = jnp.where(left, across_lanes(a), b)
            zbuf[:, pl.ds(pl.multiple_of(c * LANES, LANES), LANES)] = jnp.concatenate([low, high], axis=0).astype(jnp.bfloat16)
            return z

        lax.fori_loop(0, chips, join, 0)

        def across(d, slot):
            z = lax.rem(plane + d, n_z)
            return pltpu.make_async_remote_copy(
                zbuf, zgot.at[slot], zsend.at[d], zrecv.at[slot], device_id={"expert": z}, device_id_type=MESH
            )

        for d in range(1, n_z):
            across(d, plane).start()
        orr[pl.ds(pl.multiple_of(plane * experts, experts), experts), :] = zbuf[...]

        def factors(h):
            all_sums(h).wait_recv()
            total = lax.fori_loop(0, n, lambda s, t: t + inbox[h, s], jnp.zeros((SUBS, LANES), jnp.float32))
            scale = jnp.sqrt(total)
            osg[pl.ds(h * SUBS, SUBS), :] = scale[:, :cols]
            osu[pl.ds(h * SUBS, SUBS), :] = across_lanes(scale)[:, :cols]
            share = 1.0 / (SPAN * scale)

            def one(s, z):
                f = jnp.sqrt(inbox[h, s]) * share
                r = pltpu.roll(f, few, axis=0)
                factor[s, 0] = jnp.where(upper, f, r)
                factor[s, 1] = jnp.where(upper, r, f)
                return z

            lax.fori_loop(0, n, one, 0)

        pick = jnp.where(left, 0, half_lane) + jnp.where(upper, 0, 1)

        def decode(h):
            def chip(i, z):
                dc = lax.rem(START // 2 + MIX * i, chips)
                y = lax.rem(my_y - dc // n_x + n_y, n_y)
                x = lax.rem(my_x - dc % n_x + n_x, n_x)
                at = y * n_x + x
                for k in range(2):
                    @pl.when(2 * at + k != me)
                    def arrival():
                        for b in range(2):
                            piece_from(2 * h + b, 2 * at + k).wait_recv()

                lanes_out = pl.ds(pl.multiple_of(at * LANES, LANES), LANES)

                def values(b, k, p):
                    v = got[2 * h + b, 2 * at + k, pl.ds(p * 16, 16), :].astype(jnp.float32)
                    f = factor[2 * at + k, b]
                    out = []
                    for r in range(2):
                        w = v[r * SUBS:(r + 1) * SUBS]
                        mul = jnp.take_along_axis(f, pick + (4 * p + 2 * r), axis=1)
                        x = (jnp.log2(jnp.abs(w)) + FLOOR) * mul
                        out.append(jnp.where(w < 0, -x, x))
                    return out

                for p in range(cols // 4):
                    parts = []
                    for b in range(2):
                        one, two = values(b, 0, p), values(b, 1, p)
                        sides = []
                        for r in range(2):
                            turned = across_lanes(jnp.where(left, two[r], one[r]))
                            sides.append((jnp.where(left, one[r], turned), jnp.where(left, turned, two[r])))
                        parts.append(sides)
                    for r in range(2):
                        for t, out in ((0, og), (1, ou)):
                            a, b = parts[0][r][t], parts[1][r][t]
                            turned = pltpu.roll(jnp.where(upper, b, a), few, axis=0)
                            j = 4 * p + 2 * r
                            out[j, pl.ds(h * SUBS, SUBS), lanes_out] = jnp.where(upper, a, turned).astype(jnp.bfloat16)
                            out[j + 1, pl.ds(h * SUBS, SUBS), lanes_out] = jnp.where(upper, turned, b).astype(jnp.bfloat16)
                return z

            lax.fori_loop(0, chips, chip, 0)

        for h in range(2):
            factors(h)
            for b in range(2):
                own(2 * h + b).wait()
            decode(h)

        for d in range(1, n_z):
            z = lax.rem(plane + d, n_z)
            across(d, plane).wait_send()
            across(d, z).wait_recv()
            orr[pl.ds(pl.multiple_of(z * experts, experts), experts), :] = zgot[z]
        to_partner(my_k).wait_send()
        all_tiles().wait_send()
        for h in range(2):
            all_sums(h).wait_send()
        for a in range(QUARTERS):
            all_pieces(a).wait_send()

    return kernel


def in_hbm(array):
    return pltpu.with_memory_space_constraint(array, pltpu.HBM)


def put_out(*refs):
    n = len(refs) // 2
    sems = refs[-1]
    copies = [pltpu.make_async_copy(refs[i], refs[n + i], sems.at[i]) for i in range(n)]
    for c in copies:
        c.start()
    for c in copies:
        c.wait()


def solution(mesh):
    n_z, n = mesh.shape["expert"], mesh.shape["shard"]
    n_y = n_x = 4

    def local(master_gate, master_up, router_weight, router_gain):
        experts, rows, width = master_gate.shape
        cols = width // n
        depth = rows * n
        few = experts // QUARTERS
        f32, bf16 = jnp.float32, jnp.bfloat16
        vmem = pl.BlockSpec(memory_space=pltpu.VMEM)
        hbm = pl.BlockSpec(memory_space=pltpu.HBM)
        dma = pltpu.SemaphoreType.DMA
        shapes = (
            jax.ShapeDtypeStruct((cols, experts, depth), bf16),
            jax.ShapeDtypeStruct((cols, experts, depth), bf16),
            jax.ShapeDtypeStruct((experts, cols), f32),
            jax.ShapeDtypeStruct((experts, cols), f32),
            jax.ShapeDtypeStruct((experts * n_z, depth), bf16),
        )
        results = pl.pallas_call(
            make_kernel(experts, rows, width, cols, n_y, n_x, n_z),
            out_shape=shapes,
            in_specs=[hbm] * 4,
            out_specs=(vmem,) * 5,
            scratch_shapes=[
                pltpu.VMEM((experts, rows, width), f32),
                pltpu.VMEM((experts, rows, width), f32),
                pltpu.VMEM((LANES * few, LANES), f32),
                pltpu.VMEM((QUARTERS, width * few, LANES), bf16),
                pltpu.VMEM((QUARTERS, n, cols * few, LANES), bf16),
                pltpu.VMEM((2, 2, SUBS, width + LANES), f32),
                pltpu.VMEM((2, n, SUBS, LANES), f32),
                pltpu.VMEM((2, n, SUBS, LANES), f32),
                pltpu.VMEM((n, 2, SUBS, LANES), f32),
                pltpu.VMEM((experts, rows), f32),
                pltpu.VMEM((1, rows), f32),
                pltpu.VMEM((SUBS, LANES), bf16),
                pltpu.VMEM((2, n // 2, SUBS, LANES), bf16),
                pltpu.VMEM((experts, depth), bf16),
                pltpu.VMEM((n_z, experts, depth), bf16),
                dma((QUARTERS, 2)), dma((2,)), dma((QUARTERS,)), dma((QUARTERS,)), dma((QUARTERS, n)), dma((2,)), dma((2,)),
                dma, dma, dma((2,)), dma((n_z,)), dma((n_z,)),
            ],
            compiler_params=pltpu.CompilerParams(
                collective_id=0, has_side_effects=True, vmem_limit_bytes=48 * 2**20
            ),
        )(master_gate, master_up, in_hbm(router_weight.T), in_hbm(router_gain[None, :]))
        og, ou, osg, osu, orr = pl.pallas_call(
            put_out,
            out_shape=shapes,
            in_specs=[pl.BlockSpec(memory_space=pl.ANY)] * 5,
            out_specs=(hbm,) * 5,
            scratch_shapes=[dma((5,))],
            compiler_params=pltpu.CompilerParams(vmem_limit_bytes=2**20),
        )(*results)
        return og.transpose(1, 2, 0), ou.transpose(1, 2, 0), osg, osu, orr.T

    in_specs = (P("expert", "shard", None), P("expert", "shard", None), P("shard", "expert"), P("shard"))
    out_specs = (P("expert", None, "shard"), P("expert", None, "shard"), P("expert", "shard"), P("expert", "shard"), P())
    return jax.shard_map(local, mesh=mesh, in_specs=in_specs, out_specs=out_specs, check_vma=False)
```

```python
import jax
import jax.numpy as jnp
from jax import lax
from jax.experimental import pallas as pl
from jax.experimental.pallas import tpu as pltpu
from jax.sharding import PartitionSpec as P

MESH = pl.DeviceIdType.MESH
LANES = 128
SUBS = 8
SPAN = 250.0
FLOOR = 124.0
MIX, START = 11, 16
PARTS = (24, 20)


def encoded(x, partial):
    rate = jnp.where(partial > 0, SPAN * lax.rsqrt(partial), 0.0)
    code = jnp.exp2(jnp.abs(x) * rate - FLOOR)
    return jnp.where(x < 0, -code, code)


def make_kernel(experts, rows, width, cols, n_y, n_x, n_z):
    n = n_y * n_x * 2
    chips = n // 2
    few = SUBS // 2
    blocks = width // LANES
    half_lane = LANES // 2
    pieces = [(0, 0, cols * few), (1, 0, cols * few)]
    for i in range(len(PARTS)):
        pieces.append((2, sum(PARTS[:i]) * SUBS, PARTS[i] * SUBS))

    def kernel(gate, up, router, gain, og, ou, osg, osu, orr,
               xg, xu, stage, code_a, code_b, code_c, got_a, got_b, got_c, sums, msg, inbox, share, spread,
               xr, xgain, rtile, rin, zbuf, zgot,
               in_sem, small_sem, own_sem, send_sem, recv_sem, sums_send, sums_recv, rsend, rrecv, pair_sem, zsend, zrecv):
        codes, gots = (code_a, code_b, code_c), (got_a, got_b, got_c)
        me = lax.axis_index("shard")
        plane = lax.axis_index("expert")
        my_chip, my_k = me // 2, me % 2
        my_y, my_x = my_chip // n_x, my_chip % n_x
        stretches = ((0, few), (few, few), (2 * few, SUBS))

        def load(a, t):
            src, dst = ((gate, xg), (up, xu))[t]
            at = pl.ds(*stretches[a])
            return pltpu.make_async_copy(src.at[at], dst.at[at], in_sem.at[a, t])

        small = [pltpu.make_async_copy(router, xr, small_sem.at[0]), pltpu.make_async_copy(gain, xgain, small_sem.at[1])]
        for t in range(2):
            load(0, t).start()
        for c in small:
            c.start()
        barrier = pltpu.get_barrier_semaphore()
        for d in range(1, n_z):
            pl.semaphore_signal(barrier, 1, device_id={"expert": lax.rem(plane + d, n_z)}, device_id_type=MESH)

        def chip_at(d):
            y = lax.rem(my_y + d // (2 * n_x), n_y)
            x = lax.rem(my_x + (d // 2) % n_x, n_x)
            return y * n_x + x

        order = [d for d in ((i * MIX + START) % n for i in range(n)) if d]
        peers = [chip_at(d) * 2 + lax.rem(my_k + d % 2, 2) for d in order]
        for q in peers:
            pl.semaphore_signal(barrier, 1, device_id={"shard": q}, device_id_type=MESH)
        for a in range(1, 3):
            for t in range(2):
                load(a, t).start()

        row = lax.broadcasted_iota(jnp.int32, (SUBS, LANES), 0)
        lane = lax.broadcasted_iota(jnp.int32, (SUBS, LANES), 1)
        left = lane < half_lane
        left2 = lax.broadcasted_iota(jnp.int32, (2 * SUBS, LANES), 1) < half_lane
        upper = row < few
        used = lax.rem(lane, half_lane) < cols

        def across_lanes(v):
            return pltpu.roll(v, half_lane, axis=1)

        def produce(a):
            first, count = stretches[a]
            h, e0 = first // SUBS, first % SUBS
            size = LANES * count

            def block(b, z):
                at = pl.ds(pl.multiple_of(b * LANES, LANES), LANES)
                for e in range(count):
                    g = xg[first + e, :, at]
                    u = xu[first + e, :, at]
                    pg = jnp.sum(g * g, axis=0, keepdims=True)
                    pu = jnp.sum(u * u, axis=0, keepdims=True)
                    sums[h, 0, pl.ds(e0 + e, 1), at] = pg
                    sums[h, 1, pl.ds(e0 + e, 1), at] = pu
                    both = jnp.concatenate([encoded(g, pg), encoded(u, pu)], axis=0)
                    stage[pl.ds(e, LANES, stride=count), :] = both.T
                codes[a][pl.ds(pl.multiple_of(b * size, size), size), :] = stage[pl.ds(0, size), :].astype(jnp.bfloat16)
                return z

            lax.fori_loop(0, blocks, block, 0)

        def message(h):
            def one(q, z):
                first = q * cols
                lo = pl.multiple_of(first // LANES * LANES, LANES)
                s = lax.rem(first, LANES)
                sides = []
                for t, shift in ((0, lax.rem(LANES - s, LANES)), (1, lax.rem(LANES + half_lane - s, LANES))):
                    a = pltpu.roll(sums[h, t, :, pl.ds(lo, LANES)], shift, axis=1)
                    b = pltpu.roll(sums[h, t, :, pl.ds(lo + LANES, LANES)], shift, axis=1)
                    sides.append(jnp.where(lane - t * half_lane + s < LANES, a, b))
                msg[h, q] = jnp.where(left, sides[0], sides[1])
                return z

            lax.fori_loop(0, n, one, 0)
            inbox[h, me] = msg[h, me]

        def piece_to(m, q):
            a, first, size = pieces[m]
            whole = cols * stretches[a][1]
            return pltpu.make_async_remote_copy(
                codes[a].at[pl.ds(pl.multiple_of(q * whole + first, 16), size)], gots[a].at[me, pl.ds(first, size)],
                send_sem.at[m], recv_sem.at[m, me], device_id={"shard": q}, device_id_type=MESH,
            )

        def piece_from(m, s):
            a, first, size = pieces[m]
            ref = gots[a].at[s, pl.ds(first, size)]
            return pltpu.make_async_remote_copy(
                ref, ref, send_sem.at[m], recv_sem.at[m, s], device_id={"shard": s}, device_id_type=MESH
            )

        def all_pieces(m):
            a, _, size = pieces[m]
            ref = codes[a].at[pl.ds(0, (n - 1) * size)]
            return pltpu.make_async_remote_copy(
                ref, ref, send_sem.at[m], recv_sem.at[m, 0], device_id={"shard": me}, device_id_type=MESH
            )

        def sums_to(h, q):
            return pltpu.make_async_remote_copy(
                msg.at[h, q], inbox.at[h, me], sums_send.at[h], sums_recv.at[h], device_id={"shard": q}, device_id_type=MESH
            )

        def all_sums(h):
            src, dst = msg.at[h, pl.ds(0, n - 1)], inbox.at[h, pl.ds(0, n - 1)]
            return pltpu.make_async_remote_copy(
                src, dst, sums_send.at[h], sums_recv.at[h], device_id={"shard": me}, device_id_type=MESH
            )

        def own(a):
            size = cols * stretches[a][1]
            return pltpu.make_async_copy(
                codes[a].at[pl.ds(pl.multiple_of(me * size, 16), size)], gots[a].at[me], own_sem.at[a]
            )

        def tile_to(q):
            return pltpu.make_async_remote_copy(
                rtile, rin.at[my_k, my_chip], rsend, rrecv, device_id={"shard": q}, device_id_type=MESH
            )

        def all_tiles():
            ref = rin.at[0, pl.ds(0, chips - 1)]
            return pltpu.make_async_remote_copy(ref, ref, rsend, rrecv, device_id={"shard": me}, device_id_type=MESH)

        def to_partner(k):
            return pltpu.make_async_remote_copy(
                rin.at[k], rin.at[k], pair_sem.at[0], pair_sem.at[1],
                device_id={"shard": my_chip * 2 + 1 - my_k}, device_id_type=MESH,
            )

        for a in range(3):
            for t in range(2):
                load(a, t).wait()
            produce(a)
            if a == 0:
                for c in small:
                    c.wait()
                folded = xr[...] * xgain[...]
                rtile[...] = jnp.concatenate([folded[:SUBS], folded[SUBS:]], axis=1).astype(jnp.bfloat16)
                rin[my_k, my_chip] = rtile[...]
                pl.semaphore_wait(barrier, n - 1 + n_z - 1)
            else:
                message(a - 1)
                for q in peers:
                    sums_to(a - 1, q).start()
            for m in range(len(pieces)):
                if pieces[m][0] == a:
                    for q in peers:
                        piece_to(m, q).start()
            own(a).start()
            if a == 0:
                for d, q in zip(order, peers):
                    if d % 2 == 0:
                        tile_to(q).start()

        all_tiles().wait_recv()
        to_partner(my_k).start()
        to_partner(1 - my_k).wait_recv()

        def join(c, z):
            a, b = rin[0, c].astype(jnp.float32), rin[1, c].astype(jnp.float32)
            low = jnp.where(left, a, across_lanes(b))
            high = jnp.where(left, across_lanes(a), b)
            zbuf[:, pl.ds(pl.multiple_of(c * LANES, LANES), LANES)] = jnp.concatenate([low, high], axis=0).astype(jnp.bfloat16)
            return z

        lax.fori_loop(0, chips, join, 0)

        def across(d, slot):
            z = lax.rem(plane + d, n_z)
            return pltpu.make_async_remote_copy(
                zbuf, zgot.at[slot], zsend.at[d], zrecv.at[slot], device_id={"expert": z}, device_id_type=MESH
            )

        for d in range(1, n_z):
            across(d, plane).start()
        orr[pl.ds(pl.multiple_of(plane * experts, experts), experts), :] = zbuf[...]

        def factors(h):
            all_sums(h).wait_recv()
            total = lax.fori_loop(0, n, lambda s, t: t + inbox[h, s], jnp.zeros((SUBS, LANES), jnp.float32))
            scale = jnp.sqrt(total)
            osg[pl.ds(h * SUBS, SUBS), :] = scale[:, :cols]
            osu[pl.ds(h * SUBS, SUBS), :] = across_lanes(scale)[:, :cols]
            each = 1.0 / (SPAN * scale)
            some = jnp.logical_and(used, total > 0)

            def one(c, z):
                a = jnp.where(some, jnp.sqrt(inbox[h, 2 * c]) * each, 0.0)
                b = jnp.where(some, jnp.sqrt(inbox[h, 2 * c + 1]) * each, 0.0)
                turned = across_lanes(jnp.where(left, b, a))
                for t, f in ((0, jnp.where(left, a, turned)), (1, jnp.where(left, turned, b))):
                    at = pl.ds(pl.multiple_of(t * chips * SUBS + c * SUBS, SUBS), SUBS)
                    high = f.astype(jnp.bfloat16).astype(jnp.float32)
                    share[at, pl.ds(0, LANES)] = high
                    share[at, pl.ds(LANES, LANES)] = f - high
                return z

            lax.fori_loop(0, chips, one, 0)
            lhs = share[...].astype(jnp.bfloat16)
            k = lax.rem(lax.broadcasted_iota(jnp.int32, (2 * LANES, 2 * LANES), 0), LANES)
            m = lax.broadcasted_iota(jnp.int32, (2 * LANES, 2 * LANES), 1)
            source = k - m // LANES - lax.rem(m, LANES) // half_lane * half_lane

            def two(p, z):
                pick = jnp.where(source == 2 * p, 1.0, 0.0).astype(jnp.bfloat16)
                wide = jnp.dot(lhs, pick, preferred_element_type=jnp.float32)
                spread[2 * p] = wide[:, :LANES]
                spread[2 * p + 1] = wide[:, LANES:]
                return z

            lax.fori_loop(0, cols // 2, two, 0)

        def exponents(v):
            v = v.astype(jnp.float32)
            x = jnp.log2(jnp.abs(v)) + FLOOR
            return jnp.where(v < 0, -x, x)

        def merged(one, two):
            turned = across_lanes(jnp.where(left2, two, one))
            return jnp.where(left2, one, turned), jnp.where(left2, turned, two)

        def decode(ms, first, count):
            h = 0 if pieces[ms[0]][0] < 2 else 1

            def chip(i, z):
                dc = lax.rem(START // 2 + MIX * i, chips)
                y = lax.rem(my_y - dc // n_x + n_y, n_y)
                x = lax.rem(my_x - dc % n_x + n_x, n_x)
                at = y * n_x + x
                for k in range(2):
                    @pl.when(2 * at + k != me)
                    def arrival():
                        for m in ms:
                            piece_from(m, 2 * at + k).wait_recv()

                lanes_out = pl.ds(pl.multiple_of(at * LANES, LANES), LANES)

                def put(t, j, x):
                    f = spread[j, pl.ds(pl.multiple_of(t * chips * SUBS + at * SUBS, SUBS), SUBS), :]
                    (og, ou)[t][j, pl.ds(h * SUBS, SUBS), lanes_out] = (x * f).astype(jnp.bfloat16)

                if h:
                    for j in range(first, first + count, 2):
                        sides = merged(*(exponents(got_c[2 * at + k, pl.ds(j * SUBS, 2 * SUBS), :]) for k in range(2)))
                        for t in range(2):
                            for r in range(2):
                                put(t, j + r, sides[t][r * SUBS:(r + 1) * SUBS])
                else:
                    for j in range(first, first + count, 4):
                        rng = pl.ds(j * few, 2 * SUBS)
                        one = merged(*(exponents(got_a[2 * at + k, rng, :]) for k in range(2)))
                        two = merged(*(exponents(got_b[2 * at + k, rng, :]) for k in range(2)))
                        for t in range(2):
                            for r in range(2):
                                a, b = one[t][r * SUBS:(r + 1) * SUBS], two[t][r * SUBS:(r + 1) * SUBS]
                                turned = pltpu.roll(jnp.where(upper, b, a), few, axis=0)
                                put(t, j + 2 * r, jnp.where(upper, a, turned))
                                put(t, j + 2 * r + 1, jnp.where(upper, turned, b))
                return z

            lax.fori_loop(0, chips, chip, 0)

        factors(0)
        own(0).wait()
        own(1).wait()
        decode((0, 1), 0, cols)
        factors(1)
        own(2).wait()
        for i in range(len(PARTS)):
            decode((2 + i,), sum(PARTS[:i]), PARTS[i])

        for d in range(1, n_z):
            z = lax.rem(plane + d, n_z)
            across(d, plane).wait_send()
            across(d, z).wait_recv()
            orr[pl.ds(pl.multiple_of(z * experts, experts), experts), :] = zgot[z]
        to_partner(my_k).wait_send()
        all_tiles().wait_send()
        for h in range(2):
            all_sums(h).wait_send()
        for m in range(len(pieces)):
            all_pieces(m).wait_send()

    return kernel


def in_hbm(array):
    return pltpu.with_memory_space_constraint(array, pltpu.HBM)


def put_out(*refs):
    n = len(refs) // 2
    sems = refs[-1]
    copies = [pltpu.make_async_copy(refs[i], refs[n + i], sems.at[i]) for i in range(n)]
    for c in copies:
        c.start()
    for c in copies:
        c.wait()


def solution(mesh):
    n_z, n = mesh.shape["expert"], mesh.shape["shard"]
    n_y = n_x = 4

    def local(master_gate, master_up, router_weight, router_gain):
        experts, rows, width = master_gate.shape
        cols = width // n
        depth = rows * n
        few = SUBS // 2
        sent = 2 + len(PARTS)
        f32, bf16 = jnp.float32, jnp.bfloat16
        vmem = pl.BlockSpec(memory_space=pltpu.VMEM)
        hbm = pl.BlockSpec(memory_space=pltpu.HBM)
        dma = pltpu.SemaphoreType.DMA
        shapes = (
            jax.ShapeDtypeStruct((cols, experts, depth), bf16),
            jax.ShapeDtypeStruct((cols, experts, depth), bf16),
            jax.ShapeDtypeStruct((experts, cols), f32),
            jax.ShapeDtypeStruct((experts, cols), f32),
            jax.ShapeDtypeStruct((experts * n_z, depth), bf16),
        )
        results = pl.pallas_call(
            make_kernel(experts, rows, width, cols, n_y, n_x, n_z),
            out_shape=shapes,
            in_specs=[hbm] * 4,
            out_specs=(vmem,) * 5,
            scratch_shapes=[
                pltpu.VMEM((experts, rows, width), f32),
                pltpu.VMEM((experts, rows, width), f32),
                pltpu.VMEM((LANES * SUBS, LANES), f32),
                pltpu.VMEM((width * few, LANES), bf16),
                pltpu.VMEM((width * few, LANES), bf16),
                pltpu.VMEM((width * SUBS, LANES), bf16),
                pltpu.VMEM((n, cols * few, LANES), bf16),
                pltpu.VMEM((n, cols * few, LANES), bf16),
                pltpu.VMEM((n, cols * SUBS, LANES), bf16),
                pltpu.VMEM((2, 2, SUBS, width + LANES), f32),
                pltpu.VMEM((2, n, SUBS, LANES), f32),
                pltpu.VMEM((2, n, SUBS, LANES), f32),
                pltpu.VMEM((n * SUBS, 2 * LANES), f32),
                pltpu.VMEM((cols, n * SUBS, LANES), f32),
                pltpu.VMEM((experts, rows), f32),
                pltpu.VMEM((1, rows), f32),
                pltpu.VMEM((SUBS, LANES), bf16),
                pltpu.VMEM((2, n // 2, SUBS, LANES), bf16),
                pltpu.VMEM((experts, depth), bf16),
                pltpu.VMEM((n_z, experts, depth), bf16),
                dma((3, 2)), dma((2,)), dma((3,)), dma((sent,)), dma((sent, n)), dma((2,)), dma((2,)),
                dma, dma, dma((2,)), dma((n_z,)), dma((n_z,)),
            ],
            compiler_params=pltpu.CompilerParams(
                collective_id=0, has_side_effects=True, vmem_limit_bytes=48 * 2**20
            ),
        )(master_gate, master_up, in_hbm(router_weight.T), in_hbm(router_gain[None, :]))
        og, ou, osg, osu, orr = pl.pallas_call(
            put_out,
            out_shape=shapes,
            in_specs=[pl.BlockSpec(memory_space=pl.ANY)] * 5,
            out_specs=(hbm,) * 5,
            scratch_shapes=[dma((5,))],
            compiler_params=pltpu.CompilerParams(vmem_limit_bytes=2**20),
        )(*results)
        return og.transpose(1, 2, 0), ou.transpose(1, 2, 0), osg, osu, orr.T

    in_specs = (P("expert", "shard", None), P("expert", "shard", None), P("shard", "expert"), P("shard"))
    out_specs = (P("expert", None, "shard"), P("expert", None, "shard"), P("expert", "shard"), P("expert", "shard"), P())
    return jax.shard_map(local, mesh=mesh, in_specs=in_specs, out_specs=out_specs, check_vma=False)
```

```python
import jax
import jax.numpy as jnp
from jax import lax
from jax.experimental import pallas as pl
from jax.experimental.pallas import tpu as pltpu
from jax.sharding import PartitionSpec as P

MESH = pl.DeviceIdType.MESH
LANES = 128
SUBS = 8
SPAN = 250.0
FLOOR = 124.0
MIX, START = 11, 16
PARTS = (24, 20)


def encoded(x, partial):
    rate = jnp.where(partial > 0, SPAN * lax.rsqrt(partial), 0.0)
    code = jnp.exp2(jnp.abs(x) * rate - FLOOR)
    return jnp.where(x < 0, -code, code)


def make_kernel(experts, rows, width, cols, n_y, n_x, n_z):
    n = n_y * n_x * 2
    chips = n // 2
    few = SUBS // 2
    blocks = width // LANES
    half_lane = LANES // 2
    tile = 2 * SUBS
    pieces = [(0, 0, cols * few), (1, 0, cols * few + 2 * tile)]
    for i in range(len(PARTS)):
        pieces.append((2, sum(PARTS[:i]) * SUBS, PARTS[i] * SUBS))

    def kernel(gate, up, router, gain, og, ou, osg, osu, orr,
               xg, xu, stage, code_a, code_b, code_c, got_a, got_b, got_c, sums, share, spread,
               xr, xgain, rtile, rin, zbuf, zgot,
               in_sem, small_sem, own_sem, send_sem, recv_sem, rsend, rrecv, pair_sem, zsend, zrecv):
        codes, gots = (code_a, code_b, code_c), (got_a, got_b, got_c)
        me = lax.axis_index("shard")
        plane = lax.axis_index("expert")
        my_chip, my_k = me // 2, me % 2
        my_y, my_x = my_chip // n_x, my_chip % n_x
        stretches = ((0, few), (few, few), (2 * few, SUBS))

        def load(a, t):
            src, dst = ((gate, xg), (up, xu))[t]
            at = pl.ds(*stretches[a])
            return pltpu.make_async_copy(src.at[at], dst.at[at], in_sem.at[a, t])

        small = [pltpu.make_async_copy(router, xr, small_sem.at[0]), pltpu.make_async_copy(gain, xgain, small_sem.at[1])]
        def chip_at(d):
            y = lax.rem(my_y + d // (2 * n_x), n_y)
            x = lax.rem(my_x + (d // 2) % n_x, n_x)
            return y * n_x + x

        def hops(d):
            y, x = d // (2 * n_x), (d // 2) % n_x
            return min(y, n_y - y) + min(x, n_x - x)

        order = [d for d in ((i * MIX + START) % n for i in range(n)) if d]
        peers = [chip_at(d) * 2 + lax.rem(my_k + d % 2, 2) for d in order]
        barrier = pltpu.get_barrier_semaphore()
        for far in range(n_y // 2 + n_x // 2, -1, -1):
            for d, q in zip(order, peers):
                if hops(d) == far:
                    pl.semaphore_signal(barrier, 1, device_id={"shard": q}, device_id_type=MESH)
            if far == 4:
                for t in range(2):
                    load(0, t).start()
        for d in range(1, n_z):
            pl.semaphore_signal(barrier, 1, device_id={"expert": lax.rem(plane + d, n_z)}, device_id_type=MESH)
        for c in small:
            c.start()
        for a in range(1, 3):
            for t in range(2):
                load(a, t).start()

        row = lax.broadcasted_iota(jnp.int32, (SUBS, LANES), 0)
        lane = lax.broadcasted_iota(jnp.int32, (SUBS, LANES), 1)
        left = lane < half_lane
        left2 = lax.broadcasted_iota(jnp.int32, (2 * SUBS, LANES), 1) < half_lane
        upper = row < few
        used = lax.rem(lane, half_lane) < cols

        def across_lanes(v):
            return pltpu.roll(v, half_lane, axis=1)

        def produce(a):
            first, count = stretches[a]
            h, e0 = first // SUBS, first % SUBS
            size = LANES * count

            def block(b, z):
                at = pl.ds(pl.multiple_of(b * LANES, LANES), LANES)
                for e in range(count):
                    g = xg[first + e, :, at]
                    u = xu[first + e, :, at]
                    pg = jnp.sum(g * g, axis=0, keepdims=True)
                    pu = jnp.sum(u * u, axis=0, keepdims=True)
                    sums[h, 0, pl.ds(e0 + e, 1), at] = pg
                    sums[h, 1, pl.ds(e0 + e, 1), at] = pu
                    both = jnp.concatenate([encoded(g, pg), encoded(u, pu)], axis=0)
                    stage[pl.ds(pl.multiple_of(b * size, size) + e, LANES, stride=count), :] = both.T
                return z

            lax.fori_loop(0, blocks, block, 0)
            own_rows = cols * count

            def pack(q, z):
                rows_q = stage[pl.ds(pl.multiple_of(q * own_rows, 16), own_rows), :]
                codes[a][q, pl.ds(0, own_rows), :] = rows_q.astype(jnp.bfloat16)
                return z

            lax.fori_loop(0, n, pack, 0)

        def attach_sums():
            def one(q, z):
                first = q * cols
                lo = pl.multiple_of(first // LANES * LANES, LANES)
                s = lax.rem(first, LANES)
                for h in range(2):
                    sides = []
                    for t, shift in ((0, lax.rem(LANES - s, LANES)), (1, lax.rem(LANES + half_lane - s, LANES))):
                        a = pltpu.roll(sums[h, t, :, pl.ds(lo, LANES)], shift, axis=1)
                        b = pltpu.roll(sums[h, t, :, pl.ds(lo + LANES, LANES)], shift, axis=1)
                        sides.append(jnp.where(lane - t * half_lane + s < LANES, a, b))
                    p = jnp.where(left, sides[0], sides[1])
                    high = p.astype(jnp.bfloat16).astype(jnp.float32)
                    parts = jnp.concatenate([high, p - high], axis=0).astype(jnp.bfloat16)
                    code_b[q, pl.ds(cols * few + h * tile, tile), :] = parts
                return z

            lax.fori_loop(0, n, one, 0)

        def partial(h, s):
            parts = got_b[s, pl.ds(cols * few + h * tile, tile), :].astype(jnp.float32)
            return parts[:SUBS] + parts[SUBS:]

        def piece_to(m, q):
            a, first, size = pieces[m]
            at = pl.ds(first, size)
            return pltpu.make_async_remote_copy(
                codes[a].at[q, at], gots[a].at[me, at],
                send_sem.at[m], recv_sem.at[m, me], device_id={"shard": q}, device_id_type=MESH,
            )

        def piece_from(m, s):
            a, first, size = pieces[m]
            ref = gots[a].at[s, pl.ds(first, size)]
            return pltpu.make_async_remote_copy(
                ref, ref, send_sem.at[m], recv_sem.at[m, s], device_id={"shard": s}, device_id_type=MESH
            )

        def all_pieces(m):
            a, _, size = pieces[m]
            ref = codes[a].at[pl.ds(0, n - 1), pl.ds(0, size)]
            return pltpu.make_async_remote_copy(
                ref, ref, send_sem.at[m], recv_sem.at[m, 0], device_id={"shard": me}, device_id_type=MESH
            )

        def own(a):
            return pltpu.make_async_copy(codes[a].at[me], gots[a].at[me], own_sem.at[a])

        def tile_to(q):
            return pltpu.make_async_remote_copy(
                rtile, rin.at[my_k, my_chip], rsend, rrecv, device_id={"shard": q}, device_id_type=MESH
            )

        def all_tiles():
            ref = rin.at[0, pl.ds(0, chips - 1)]
            return pltpu.make_async_remote_copy(ref, ref, rsend, rrecv, device_id={"shard": me}, device_id_type=MESH)

        def to_partner(k):
            return pltpu.make_async_remote_copy(
                rin.at[k], rin.at[k], pair_sem.at[0], pair_sem.at[1],
                device_id={"shard": my_chip * 2 + 1 - my_k}, device_id_type=MESH,
            )

        def send(m):
            for q in peers:
                piece_to(m, q).start()

        for a in range(3):
            for t in range(2):
                load(a, t).wait()
            produce(a)
            if a == 0:
                for c in small:
                    c.wait()
                folded = xr[...] * xgain[...]
                rtile[...] = jnp.concatenate([folded[:SUBS], folded[SUBS:]], axis=1).astype(jnp.bfloat16)
                rin[my_k, my_chip] = rtile[...]
                pl.semaphore_wait(barrier, n - 1 + n_z - 1)
                send(0)
                for d, q in zip(order, peers):
                    if d % 2 == 0:
                        tile_to(q).start()
        attach_sums()
        for m in range(1, len(pieces)):
            send(m)
        for a in range(3):
            own(a).start()

        all_tiles().wait_recv()
        to_partner(my_k).start()
        to_partner(1 - my_k).wait_recv()

        def join(c, z):
            a, b = rin[0, c].astype(jnp.float32), rin[1, c].astype(jnp.float32)
            low = jnp.where(left, a, across_lanes(b))
            high = jnp.where(left, across_lanes(a), b)
            zbuf[:, pl.ds(pl.multiple_of(c * LANES, LANES), LANES)] = jnp.concatenate([low, high], axis=0).astype(jnp.bfloat16)
            return z

        lax.fori_loop(0, chips, join, 0)

        def across(d, slot):
            z = lax.rem(plane + d, n_z)
            return pltpu.make_async_remote_copy(
                zbuf, zgot.at[slot], zsend.at[d], zrecv.at[slot], device_id={"expert": z}, device_id_type=MESH
            )

        for d in range(1, n_z):
            across(d, plane).start()
        orr[pl.ds(pl.multiple_of(plane * experts, experts), experts), :] = zbuf[...]

        def factors(h):
            total = lax.fori_loop(0, n, lambda s, t: t + partial(h, s), jnp.zeros((SUBS, LANES), jnp.float32))
            scale = jnp.sqrt(total)
            osg[pl.ds(h * SUBS, SUBS), :] = scale[:, :cols]
            osu[pl.ds(h * SUBS, SUBS), :] = across_lanes(scale)[:, :cols]
            each = 1.0 / (SPAN * scale)
            some = jnp.logical_and(used, total > 0)

            def one(c, z):
                a = jnp.where(some, jnp.sqrt(partial(h, 2 * c)) * each, 0.0)
                b = jnp.where(some, jnp.sqrt(partial(h, 2 * c + 1)) * each, 0.0)
                turned = across_lanes(jnp.where(left, b, a))
                for t, f in ((0, jnp.where(left, a, turned)), (1, jnp.where(left, turned, b))):
                    at = pl.ds(pl.multiple_of(t * chips * SUBS + c * SUBS, SUBS), SUBS)
                    high = f.astype(jnp.bfloat16).astype(jnp.float32)
                    share[at, pl.ds(0, LANES)] = high
                    share[at, pl.ds(LANES, LANES)] = f - high
                return z

            lax.fori_loop(0, chips, one, 0)
            lhs = share[...].astype(jnp.bfloat16)
            k = lax.rem(lax.broadcasted_iota(jnp.int32, (2 * LANES, 2 * LANES), 0), LANES)
            m = lax.broadcasted_iota(jnp.int32, (2 * LANES, 2 * LANES), 1)
            source = k - m // LANES - lax.rem(m, LANES) // half_lane * half_lane

            def two(p, z):
                pick = jnp.where(source == 2 * p, 1.0, 0.0).astype(jnp.bfloat16)
                wide = jnp.dot(lhs, pick, preferred_element_type=jnp.float32)
                spread[h, 2 * p] = wide[:, :LANES]
                spread[h, 2 * p + 1] = wide[:, LANES:]
                return z

            lax.fori_loop(0, cols // 2, two, 0)

        def exponents(v):
            v = v.astype(jnp.float32)
            x = jnp.log2(jnp.abs(v)) + FLOOR
            return jnp.where(v < 0, -x, x)

        def merged(one, two):
            turned = across_lanes(jnp.where(left2, two, one))
            return jnp.where(left2, one, turned), jnp.where(left2, turned, two)

        def decode(m, first, count):
            h = pieces[m][0] // 2

            def chip(i, z):
                dc = lax.rem(START // 2 + MIX * i, chips)
                y = lax.rem(my_y - dc // n_x + n_y, n_y)
                x = lax.rem(my_x - dc % n_x + n_x, n_x)
                at = y * n_x + x
                for k in range(2):
                    @pl.when(2 * at + k != me)
                    def arrival():
                        piece_from(m, 2 * at + k).wait_recv()

                lanes_out = pl.ds(pl.multiple_of(at * LANES, LANES), LANES)

                def put(t, j, x):
                    f = spread[h, j, pl.ds(pl.multiple_of(t * chips * SUBS + at * SUBS, SUBS), SUBS), :]
                    (og, ou)[t][j, pl.ds(h * SUBS, SUBS), lanes_out] = (x * f).astype(jnp.bfloat16)

                if h:
                    for j in range(first, first + count, 2):
                        sides = merged(*(exponents(got_c[2 * at + k, pl.ds(j * SUBS, 2 * SUBS), :]) for k in range(2)))
                        for t in range(2):
                            for r in range(2):
                                put(t, j + r, sides[t][r * SUBS:(r + 1) * SUBS])
                else:
                    for j in range(first, first + count, 4):
                        rng = pl.ds(j * few, 2 * SUBS)
                        one = merged(*(exponents(got_a[2 * at + k, rng, :]) for k in range(2)))
                        two = merged(*(exponents(got_b[2 * at + k, rng, :]) for k in range(2)))
                        for t in range(2):
                            for r in range(2):
                                a, b = one[t][r * SUBS:(r + 1) * SUBS], two[t][r * SUBS:(r + 1) * SUBS]
                                turned = pltpu.roll(jnp.where(upper, b, a), few, axis=0)
                                put(t, j + 2 * r, jnp.where(upper, a, turned))
                                put(t, j + 2 * r + 1, jnp.where(upper, turned, b))
                return z

            lax.fori_loop(0, chips, chip, 0)

        for a in range(3):
            own(a).wait()
        for q in peers:
            piece_from(1, q).wait_recv()
        factors(0)
        decode(0, 0, cols)
        factors(1)
        for d in range(1, n_z):
            z = lax.rem(plane + d, n_z)
            across(d, plane).wait_send()
            across(d, z).wait_recv()
            orr[pl.ds(pl.multiple_of(z * experts, experts), experts), :] = zgot[z]
        to_partner(my_k).wait_send()
        all_tiles().wait_send()
        for i in range(len(PARTS)):
            decode(2 + i, sum(PARTS[:i]), PARTS[i])
        for m in range(len(pieces)):
            all_pieces(m).wait_send()

    return kernel


def in_hbm(array):
    return pltpu.with_memory_space_constraint(array, pltpu.HBM)


def put_out(*refs):
    n = len(refs) // 2
    sems = refs[-1]
    copies = [pltpu.make_async_copy(refs[i], refs[n + i], sems.at[i]) for i in range(n)]
    for c in copies:
        c.start()
    for c in copies:
        c.wait()


def solution(mesh):
    n_z, n = mesh.shape["expert"], mesh.shape["shard"]
    n_y = n_x = 4

    def local(master_gate, master_up, router_weight, router_gain):
        experts, rows, width = master_gate.shape
        cols = width // n
        depth = rows * n
        few = SUBS // 2
        sent = 2 + len(PARTS)
        f32, bf16 = jnp.float32, jnp.bfloat16
        vmem = pl.BlockSpec(memory_space=pltpu.VMEM)
        hbm = pl.BlockSpec(memory_space=pltpu.HBM)
        dma = pltpu.SemaphoreType.DMA
        shapes = (
            jax.ShapeDtypeStruct((cols, experts, depth), bf16),
            jax.ShapeDtypeStruct((cols, experts, depth), bf16),
            jax.ShapeDtypeStruct((experts, cols), f32),
            jax.ShapeDtypeStruct((experts, cols), f32),
            jax.ShapeDtypeStruct((experts * n_z, depth), bf16),
        )
        results = pl.pallas_call(
            make_kernel(experts, rows, width, cols, n_y, n_x, n_z),
            out_shape=shapes,
            in_specs=[hbm] * 4,
            out_specs=(vmem,) * 5,
            scratch_shapes=[
                pltpu.VMEM((experts, rows, width), f32),
                pltpu.VMEM((experts, rows, width), f32),
                pltpu.VMEM((width * SUBS, LANES), f32),
                *[pltpu.VMEM((n, r, LANES), bf16) for r in (cols * few, cols * few + 4 * SUBS, cols * SUBS)] * 2,
                pltpu.VMEM((2, 2, SUBS, width + LANES), f32),
                pltpu.VMEM((n * SUBS, 2 * LANES), f32),
                pltpu.VMEM((2, cols, n * SUBS, LANES), f32),
                pltpu.VMEM((experts, rows), f32),
                pltpu.VMEM((1, rows), f32),
                pltpu.VMEM((SUBS, LANES), bf16),
                pltpu.VMEM((2, n // 2, SUBS, LANES), bf16),
                pltpu.VMEM((experts, depth), bf16),
                pltpu.VMEM((n_z, experts, depth), bf16),
                dma((3, 2)), dma((2,)), dma((3,)), dma((sent,)), dma((sent, n)),
                dma, dma, dma((2,)), dma((n_z,)), dma((n_z,)),
            ],
            compiler_params=pltpu.CompilerParams(
                collective_id=0, has_side_effects=True, vmem_limit_bytes=45 * 2**20
            ),
        )(master_gate, master_up, in_hbm(router_weight.T), in_hbm(router_gain[None, :]))
        og, ou, osg, osu, orr = pl.pallas_call(
            put_out,
            out_shape=shapes,
            in_specs=[pl.BlockSpec(memory_space=pl.ANY)] * 5,
            out_specs=(hbm,) * 5,
            scratch_shapes=[dma((5,))],
            compiler_params=pltpu.CompilerParams(vmem_limit_bytes=2**20),
        )(*results)
        return og.transpose(1, 2, 0), ou.transpose(1, 2, 0), osg, osu, orr.T

    in_specs = (P("expert", "shard", None), P("expert", "shard", None), P("shard", "expert"), P("shard"))
    out_specs = (P("expert", None, "shard"), P("expert", None, "shard"), P("expert", "shard"), P("expert", "shard"), P())
    return jax.shard_map(local, mesh=mesh, in_specs=in_specs, out_specs=out_specs, check_vma=False)
```

```python
import jax
import jax.numpy as jnp
from jax import lax
from jax.experimental import pallas as pl
from jax.experimental.pallas import tpu as pltpu
from jax.sharding import PartitionSpec as P

MESH = pl.DeviceIdType.MESH
LANES = 128
SUBS = 8
SPAN = 250.0
FLOOR = 124.0
MIX, START = 23, 16
PARTS = (24, 20)


def encoded(x, partial):
    rate = jnp.where(partial > 0, SPAN * lax.rsqrt(partial), 0.0)
    code = jnp.exp2(jnp.abs(x) * rate - FLOOR)
    return jnp.where(x < 0, -code, code)


def make_kernel(experts, rows, width, cols, n_y, n_x, n_z):
    n = n_y * n_x * 2
    chips = n // 2
    few = SUBS // 2
    blocks = width // LANES
    half_lane = LANES // 2
    tile = 2 * SUBS
    pieces = [(0, 0, cols * few), (1, 0, cols * few + 2 * tile)]
    for i in range(len(PARTS)):
        pieces.append((2, sum(PARTS[:i]) * SUBS, PARTS[i] * SUBS))

    def kernel(gate, up, router, gain, og, ou, osg, osu, orr,
               xg, xu, stage, code_a, code_b, code_c, got_a, got_b, got_c, sums, share, spread,
               xr, xgain, zbuf, zgot,
               in_sem, small_sem, own_sem, send_sem, recv_sem, zsend, zrecv):
        codes, gots = (code_a, code_b, code_c), (got_a, got_b, got_c)
        me = lax.axis_index("shard")
        plane = lax.axis_index("expert")
        my_chip, my_k = me // 2, me % 2
        my_y, my_x = my_chip // n_x, my_chip % n_x
        stretches = ((0, few), (few, few), (2 * few, SUBS))

        def load(a, t):
            src, dst = ((gate, xg), (up, xu))[t]
            at = pl.ds(*stretches[a])
            return pltpu.make_async_copy(src.at[at], dst.at[at], in_sem.at[a, t])

        small = [pltpu.make_async_copy(router, xr, small_sem.at[0]), pltpu.make_async_copy(gain, xgain, small_sem.at[1])]
        def chip_at(d):
            y = lax.rem(my_y + d // (2 * n_x), n_y)
            x = lax.rem(my_x + (d // 2) % n_x, n_x)
            return y * n_x + x

        def hops(d):
            y, x = d // (2 * n_x), (d // 2) % n_x
            return min(y, n_y - y) + min(x, n_x - x)

        order = [d for d in ((i * MIX + START) % n for i in range(n)) if d]
        peers = [chip_at(d) * 2 + lax.rem(my_k + d % 2, 2) for d in order]
        barrier = pltpu.get_barrier_semaphore()
        for far in range(n_y // 2 + n_x // 2, -1, -1):
            for d, q in zip(order, peers):
                if hops(d) == far:
                    pl.semaphore_signal(barrier, 1, device_id={"shard": q}, device_id_type=MESH)
            if far == 4:
                for t in range(2):
                    load(0, t).start()
        for d in range(1, n_z):
            pl.semaphore_signal(barrier, 1, device_id={"expert": lax.rem(plane + d, n_z)}, device_id_type=MESH)
        for c in small:
            c.start()
        for a in range(1, 3):
            for t in range(2):
                load(a, t).start()

        row = lax.broadcasted_iota(jnp.int32, (SUBS, LANES), 0)
        lane = lax.broadcasted_iota(jnp.int32, (SUBS, LANES), 1)
        left = lane < half_lane
        left2 = lax.broadcasted_iota(jnp.int32, (2 * SUBS, LANES), 1) < half_lane
        upper = row < few
        lane2 = lax.broadcasted_iota(jnp.int32, (2 * SUBS, LANES), 1)
        used, used2 = lax.rem(lane, half_lane) < cols, lax.rem(lane2, half_lane) < cols
        quarter = half_lane // 4

        def across_lanes(v):
            return pltpu.roll(v, half_lane, axis=1)

        def produce(a):
            first, count = stretches[a]
            h, e0 = first // SUBS, first % SUBS
            size = LANES * count

            def block(b, z):
                at = pl.ds(pl.multiple_of(b * LANES, LANES), LANES)
                for e in range(count):
                    g = xg[first + e, :, at]
                    u = xu[first + e, :, at]
                    pg = jnp.sum(g * g, axis=0, keepdims=True)
                    pu = jnp.sum(u * u, axis=0, keepdims=True)
                    sums[h, 0, pl.ds(e0 + e, 1), at] = pg
                    sums[h, 1, pl.ds(e0 + e, 1), at] = pu
                    both = jnp.concatenate([encoded(g, pg), encoded(u, pu)], axis=0)
                    stage[pl.ds(pl.multiple_of(b * size, size) + e, LANES, stride=count), :] = both.T
                return z

            lax.fori_loop(0, blocks, block, 0)
            own_rows = cols * count

            def pack(q, z):
                rows_q = stage[pl.ds(pl.multiple_of(q * own_rows, 16), own_rows), :]
                codes[a][q, pl.ds(0, own_rows), :] = rows_q.astype(jnp.bfloat16)
                return z

            lax.fori_loop(0, n, pack, 0)

        def attach_sums():
            for c in small:
                c.wait()
            folded = xr[...] * xgain[...]
            folded = jnp.concatenate([folded, folded], axis=1)
            riders = []
            for h in range(2):
                near, far = (pltpu.roll(folded, at - i * quarter, axis=1) for at, i in ((cols, 2 * h), (half_lane + cols, 2 * h + 1)))
                riders.append(jnp.where(left2, near, far))

            def one(q, z):
                first = q * cols
                lo = pl.multiple_of(first // LANES * LANES, LANES)
                s = lax.rem(first, LANES)
                for h in range(2):
                    sides = []
                    for t, shift in ((0, lax.rem(LANES - s, LANES)), (1, lax.rem(LANES + half_lane - s, LANES))):
                        a = pltpu.roll(sums[h, t, :, pl.ds(lo, LANES)], shift, axis=1)
                        b = pltpu.roll(sums[h, t, :, pl.ds(lo + LANES, LANES)], shift, axis=1)
                        sides.append(jnp.where(lane - t * half_lane + s < LANES, a, b))
                    p = jnp.where(left, sides[0], sides[1])
                    high = p.astype(jnp.bfloat16).astype(jnp.float32)
                    parts = jnp.where(used2, jnp.concatenate([high, p - high], axis=0), riders[h])
                    code_b[q, pl.ds(cols * few + h * tile, tile), :] = parts.astype(jnp.bfloat16)
                return z

            lax.fori_loop(0, n, one, 0)

        def partial(h, s):
            parts = got_b[s, pl.ds(cols * few + h * tile, tile), :].astype(jnp.float32)
            return parts[:SUBS] + parts[SUBS:]

        def piece_to(m, q):
            a, first, size = pieces[m]
            at = pl.ds(first, size)
            return pltpu.make_async_remote_copy(
                codes[a].at[q, at], gots[a].at[me, at],
                send_sem.at[m], recv_sem.at[m, me], device_id={"shard": q}, device_id_type=MESH,
            )

        def piece_from(m, s):
            a, first, size = pieces[m]
            ref = gots[a].at[s, pl.ds(first, size)]
            return pltpu.make_async_remote_copy(
                ref, ref, send_sem.at[m], recv_sem.at[m, s], device_id={"shard": s}, device_id_type=MESH
            )

        def all_pieces(m):
            a, _, size = pieces[m]
            ref = codes[a].at[pl.ds(0, n - 1), pl.ds(0, size)]
            return pltpu.make_async_remote_copy(
                ref, ref, send_sem.at[m], recv_sem.at[m, 0], device_id={"shard": me}, device_id_type=MESH
            )

        def own(a):
            return pltpu.make_async_copy(codes[a].at[me], gots[a].at[me], own_sem.at[a])

        def send(m):
            for q in peers:
                piece_to(m, q).start()

        for a in range(3):
            for t in range(2):
                load(a, t).wait()
            produce(a)
            if a == 0:
                pl.semaphore_wait(barrier, n - 1 + n_z - 1)
                send(0)
        attach_sums()
        for m in range(1, len(pieces)):
            send(m)
        for a in range(3):
            own(a).start()

        for a in range(3):
            own(a).wait()
        for q in peers:
            piece_from(1, q).wait_recv()

        def join(c, z):
            whole = jnp.zeros((2 * SUBS, LANES), jnp.float32)
            for k in range(2):
                for h in range(2):
                    v = got_b[2 * c + k, pl.ds(cols * few + h * tile, tile), :].astype(jnp.float32)
                    for side in range(2):
                        to = k * half_lane + (2 * h + side) * quarter
                        moved = pltpu.roll(v, (to - side * half_lane - cols) % LANES, axis=1)
                        whole = jnp.where(jnp.logical_and(lane2 >= to, lane2 < to + quarter), moved, whole)
            zbuf[:, pl.ds(pl.multiple_of(c * LANES, LANES), LANES)] = whole.astype(jnp.bfloat16)
            return z

        lax.fori_loop(0, chips, join, 0)

        def across(d, slot):
            z = lax.rem(plane + d, n_z)
            return pltpu.make_async_remote_copy(
                zbuf, zgot.at[slot], zsend.at[d], zrecv.at[slot], device_id={"expert": z}, device_id_type=MESH
            )

        for d in range(1, n_z):
            across(d, plane).start()
        orr[pl.ds(pl.multiple_of(plane * experts, experts), experts), :] = zbuf[...]

        def factors(h):
            total = lax.fori_loop(0, n, lambda s, t: t + partial(h, s), jnp.zeros((SUBS, LANES), jnp.float32))
            scale = jnp.sqrt(total)
            osg[pl.ds(h * SUBS, SUBS), :] = scale[:, :cols]
            osu[pl.ds(h * SUBS, SUBS), :] = across_lanes(scale)[:, :cols]
            each = 1.0 / (SPAN * scale)
            some = jnp.logical_and(used, total > 0)

            def one(c, z):
                a = jnp.where(some, jnp.sqrt(partial(h, 2 * c)) * each, 0.0)
                b = jnp.where(some, jnp.sqrt(partial(h, 2 * c + 1)) * each, 0.0)
                turned = across_lanes(jnp.where(left, b, a))
                for t, f in ((0, jnp.where(left, a, turned)), (1, jnp.where(left, turned, b))):
                    at = pl.ds(pl.multiple_of(t * chips * SUBS + c * SUBS, SUBS), SUBS)
                    high = f.astype(jnp.bfloat16).astype(jnp.float32)
                    share[at, pl.ds(0, LANES)] = high
                    share[at, pl.ds(LANES, LANES)] = f - high
                return z

            lax.fori_loop(0, chips, one, 0)
            lhs = share[...].astype(jnp.bfloat16)
            k = lax.rem(lax.broadcasted_iota(jnp.int32, (2 * LANES, 2 * LANES), 0), LANES)
            m = lax.broadcasted_iota(jnp.int32, (2 * LANES, 2 * LANES), 1)
            source = k - m // LANES - lax.rem(m, LANES) // half_lane * half_lane

            def two(p, z):
                pick = jnp.where(source == 2 * p, 1.0, 0.0).astype(jnp.bfloat16)
                wide = jnp.dot(lhs, pick, preferred_element_type=jnp.float32)
                spread[h, 2 * p] = wide[:, :LANES]
                spread[h, 2 * p + 1] = wide[:, LANES:]
                return z

            lax.fori_loop(0, cols // 2, two, 0)

        def exponents(v):
            v = v.astype(jnp.float32)
            x = jnp.log2(jnp.abs(v)) + FLOOR
            return jnp.where(v < 0, -x, x)

        def merged(one, two):
            turned = across_lanes(jnp.where(left2, two, one))
            return jnp.where(left2, one, turned), jnp.where(left2, turned, two)

        def decode(m, first, count):
            h = pieces[m][0] // 2

            def chip(i, z):
                dc = lax.rem(START // 2 + MIX * i, chips)
                y = lax.rem(my_y - dc // n_x + n_y, n_y)
                x = lax.rem(my_x - dc % n_x + n_x, n_x)
                at = y * n_x + x
                for k in range(2):
                    @pl.when(2 * at + k != me)
                    def arrival():
                        piece_from(m, 2 * at + k).wait_recv()

                lanes_out = pl.ds(pl.multiple_of(at * LANES, LANES), LANES)

                def put(t, j, x):
                    f = spread[h, j, pl.ds(pl.multiple_of(t * chips * SUBS + at * SUBS, SUBS), SUBS), :]
                    (og, ou)[t][j, pl.ds(h * SUBS, SUBS), lanes_out] = (x * f).astype(jnp.bfloat16)

                if h:
                    for j in range(first, first + count, 2):
                        sides = merged(*(exponents(got_c[2 * at + k, pl.ds(j * SUBS, 2 * SUBS), :]) for k in range(2)))
                        for t in range(2):
                            for r in range(2):
                                put(t, j + r, sides[t][r * SUBS:(r + 1) * SUBS])
                else:
                    for j in range(first, first + count, 4):
                        rng = pl.ds(j * few, 2 * SUBS)
                        one = merged(*(exponents(got_a[2 * at + k, rng, :]) for k in range(2)))
                        two = merged(*(exponents(got_b[2 * at + k, rng, :]) for k in range(2)))
                        for t in range(2):
                            for r in range(2):
                                a, b = one[t][r * SUBS:(r + 1) * SUBS], two[t][r * SUBS:(r + 1) * SUBS]
                                turned = pltpu.roll(jnp.where(upper, b, a), few, axis=0)
                                put(t, j + 2 * r, jnp.where(upper, a, turned))
                                put(t, j + 2 * r + 1, jnp.where(upper, turned, b))
                return z

            lax.fori_loop(0, chips, chip, 0)

        factors(0)
        decode(0, 0, cols)
        factors(1)
        for d in range(1, n_z):
            z = lax.rem(plane + d, n_z)
            across(d, plane).wait_send()
            across(d, z).wait_recv()
            orr[pl.ds(pl.multiple_of(z * experts, experts), experts), :] = zgot[z]
        for i in range(len(PARTS)):
            decode(2 + i, sum(PARTS[:i]), PARTS[i])
        for m in range(len(pieces)):
            all_pieces(m).wait_send()

    return kernel


def in_hbm(array):
    return pltpu.with_memory_space_constraint(array, pltpu.HBM)


def put_out(*refs):
    n = len(refs) // 2
    sems = refs[-1]
    copies = [pltpu.make_async_copy(refs[i], refs[n + i], sems.at[i]) for i in range(n)]
    for c in copies:
        c.start()
    for c in copies:
        c.wait()


def solution(mesh):
    n_z, n = mesh.shape["expert"], mesh.shape["shard"]
    n_y = n_x = 4

    def local(master_gate, master_up, router_weight, router_gain):
        experts, rows, width = master_gate.shape
        cols = width // n
        depth = rows * n
        few = SUBS // 2
        sent = 2 + len(PARTS)
        f32, bf16 = jnp.float32, jnp.bfloat16
        vmem = pl.BlockSpec(memory_space=pltpu.VMEM)
        hbm = pl.BlockSpec(memory_space=pltpu.HBM)
        dma = pltpu.SemaphoreType.DMA
        shapes = (
            jax.ShapeDtypeStruct((cols, experts, depth), bf16),
            jax.ShapeDtypeStruct((cols, experts, depth), bf16),
            jax.ShapeDtypeStruct((experts, cols), f32),
            jax.ShapeDtypeStruct((experts, cols), f32),
            jax.ShapeDtypeStruct((experts * n_z, depth), bf16),
        )
        results = pl.pallas_call(
            make_kernel(experts, rows, width, cols, n_y, n_x, n_z),
            out_shape=shapes,
            in_specs=[hbm] * 4,
            out_specs=(vmem,) * 5,
            scratch_shapes=[
                pltpu.VMEM((experts, rows, width), f32),
                pltpu.VMEM((experts, rows, width), f32),
                pltpu.VMEM((width * SUBS + SUBS, LANES), f32),
                *[pltpu.VMEM((n, r, LANES), bf16) for r in (cols * few, cols * few + 4 * SUBS, cols * SUBS)] * 2,
                pltpu.VMEM((2, 2, SUBS, width + LANES), f32),
                pltpu.VMEM((n * SUBS, 2 * LANES), f32),
                pltpu.VMEM((2, cols, n * SUBS, LANES), f32),
                pltpu.VMEM((experts, rows), f32),
                pltpu.VMEM((1, rows), f32),
                pltpu.VMEM((experts, depth), bf16),
                pltpu.VMEM((n_z, experts, depth), bf16),
                dma((3, 2)), dma((2,)), dma((3,)), dma((sent,)), dma((sent, n)),
                dma((n_z,)), dma((n_z,)),
            ],
            compiler_params=pltpu.CompilerParams(
                collective_id=0, has_side_effects=True, vmem_limit_bytes=45 * 2**20
            ),
        )(master_gate, master_up, in_hbm(router_weight.T), in_hbm(router_gain[None, :]))
        og, ou, osg, osu, orr = pl.pallas_call(
            put_out,
            out_shape=shapes,
            in_specs=[pl.BlockSpec(memory_space=pl.ANY)] * 5,
            out_specs=(hbm,) * 5,
            scratch_shapes=[dma((5,))],
            compiler_params=pltpu.CompilerParams(vmem_limit_bytes=2**20),
        )(*results)
        return og.transpose(1, 2, 0), ou.transpose(1, 2, 0), osg, osu, orr.T

    in_specs = (P("expert", "shard", None), P("expert", "shard", None), P("shard", "expert"), P("shard"))
    out_specs = (P("expert", None, "shard"), P("expert", None, "shard"), P("expert", "shard"), P("expert", "shard"), P())
    return jax.shard_map(local, mesh=mesh, in_specs=in_specs, out_specs=out_specs, check_vma=False)
```

```python
import jax
import jax.numpy as jnp
from jax import lax
from jax.experimental import pallas as pl
from jax.experimental.pallas import tpu as pltpu
from jax.sharding import PartitionSpec as P

MESH = pl.DeviceIdType.MESH
LANES = 128
SUBS = 8
SPAN = 250.0
FLOOR = 124.0
MIX, START = 23, 8
PARTS = (24, 20)


def encoded(x, partial):
    rate = jnp.where(partial > 0, SPAN * lax.rsqrt(partial), 0.0)
    code = jnp.exp2(jnp.abs(x) * rate - FLOOR)
    return jnp.where(x < 0, -code, code)


def make_kernel(experts, rows, width, cols, n_y, n_x, n_z):
    n = n_y * n_x * 2
    chips = n // 2
    few = SUBS // 2
    blocks = width // LANES
    half_lane = LANES // 2
    tile = 2 * SUBS
    pieces = [(0, 0, cols * few), (1, 0, cols * few + 2 * tile)]
    for i in range(len(PARTS)):
        pieces.append((2, sum(PARTS[:i]) * SUBS, PARTS[i] * SUBS))

    def kernel(gate, up, router, gain, og, ou, osg, osu, orr,
               xg, xu, stage, code_a, code_b, code_c, got_a, got_b, got_c, sums, share, spread,
               xr, xgain, zbuf, zgot,
               in_sem, small_sem, own_sem, send_sem, recv_sem, zsend, zrecv):
        codes, gots = (code_a, code_b, code_c), (got_a, got_b, got_c)
        me = lax.axis_index("shard")
        plane = lax.axis_index("expert")
        my_chip, my_k = me // 2, me % 2
        my_y, my_x = my_chip // n_x, my_chip % n_x
        stretches = ((0, few), (few, few), (2 * few, SUBS))

        def load(a, t):
            src, dst = ((gate, xg), (up, xu))[t]
            at = pl.ds(*stretches[a])
            return pltpu.make_async_copy(src.at[at], dst.at[at], in_sem.at[a, t])

        small = [pltpu.make_async_copy(router, xr, small_sem.at[0]), pltpu.make_async_copy(gain, xgain, small_sem.at[1])]
        def chip_at(d):
            y = lax.rem(my_y + d // (2 * n_x), n_y)
            x = lax.rem(my_x + (d // 2) % n_x, n_x)
            return y * n_x + x

        def hops(d):
            y, x = d // (2 * n_x), (d // 2) % n_x
            return min(y, n_y - y) + min(x, n_x - x)

        order = [d for d in ((i * MIX + START) % n for i in range(n)) if d]
        peers = [chip_at(d) * 2 + lax.rem(my_k + d % 2, 2) for d in order]
        barrier = pltpu.get_barrier_semaphore()
        for far in range(n_y // 2 + n_x // 2, -1, -1):
            for d, q in zip(order, peers):
                if hops(d) == far:
                    pl.semaphore_signal(barrier, 1, device_id={"shard": q}, device_id_type=MESH)
            if far == 4:
                for t in range(2):
                    load(0, t).start()
        for d in range(1, n_z):
            pl.semaphore_signal(barrier, 1, device_id={"expert": lax.rem(plane + d, n_z)}, device_id_type=MESH)
        for c in small:
            c.start()
        for a in range(1, 3):
            for t in range(2):
                load(a, t).start()

        row = lax.broadcasted_iota(jnp.int32, (SUBS, LANES), 0)
        lane = lax.broadcasted_iota(jnp.int32, (SUBS, LANES), 1)
        left = lane < half_lane
        left2 = lax.broadcasted_iota(jnp.int32, (2 * SUBS, LANES), 1) < half_lane
        upper = row < few
        lane2 = lax.broadcasted_iota(jnp.int32, (2 * SUBS, LANES), 1)
        used, used2 = lax.rem(lane, half_lane) < cols, lax.rem(lane2, half_lane) < cols
        quarter = half_lane // 4

        def across_lanes(v):
            return pltpu.roll(v, half_lane, axis=1)

        def produce(a):
            first, count = stretches[a]
            h, e0 = first // SUBS, first % SUBS
            size = LANES * count

            def block(b, z):
                at = pl.ds(pl.multiple_of(b * LANES, LANES), LANES)
                for e in range(count):
                    g = xg[first + e, :, at]
                    u = xu[first + e, :, at]
                    pg = jnp.sum(g * g, axis=0, keepdims=True)
                    pu = jnp.sum(u * u, axis=0, keepdims=True)
                    sums[h, 0, pl.ds(e0 + e, 1), at] = pg
                    sums[h, 1, pl.ds(e0 + e, 1), at] = pu
                    both = jnp.concatenate([encoded(g, pg), encoded(u, pu)], axis=0)
                    stage[pl.ds(pl.multiple_of(b * size, size) + e, LANES, stride=count), :] = both.T
                return z

            lax.fori_loop(0, blocks, block, 0)
            own_rows = cols * count

            def pack(q, z):
                rows_q = stage[pl.ds(pl.multiple_of(q * own_rows, 16), own_rows), :]
                codes[a][q, pl.ds(0, own_rows), :] = rows_q.astype(jnp.bfloat16)
                return z

            lax.fori_loop(0, n, pack, 0)

        def attach_sums():
            for c in small:
                c.wait()
            folded = xr[...] * xgain[...]
            folded = jnp.concatenate([folded, folded], axis=1)
            riders = []
            for h in range(2):
                near, far = (pltpu.roll(folded, at - i * quarter, axis=1) for at, i in ((cols, 2 * h), (half_lane + cols, 2 * h + 1)))
                riders.append(jnp.where(left2, near, far))

            def one(q, z):
                first = q * cols
                lo = pl.multiple_of(first // LANES * LANES, LANES)
                s = lax.rem(first, LANES)
                for h in range(2):
                    sides = []
                    for t, shift in ((0, lax.rem(LANES - s, LANES)), (1, lax.rem(LANES + half_lane - s, LANES))):
                        a = pltpu.roll(sums[h, t, :, pl.ds(lo, LANES)], shift, axis=1)
                        b = pltpu.roll(sums[h, t, :, pl.ds(lo + LANES, LANES)], shift, axis=1)
                        sides.append(jnp.where(lane - t * half_lane + s < LANES, a, b))
                    p = jnp.where(left, sides[0], sides[1])
                    high = p.astype(jnp.bfloat16).astype(jnp.float32)
                    parts = jnp.where(used2, jnp.concatenate([high, p - high], axis=0), riders[h])
                    code_b[q, pl.ds(cols * few + h * tile, tile), :] = parts.astype(jnp.bfloat16)
                return z

            lax.fori_loop(0, n, one, 0)

        def partial(h, s):
            parts = got_b[s, pl.ds(cols * few + h * tile, tile), :].astype(jnp.float32)
            return parts[:SUBS] + parts[SUBS:]

        def piece_to(m, q):
            a, first, size = pieces[m]
            at = pl.ds(first, size)
            return pltpu.make_async_remote_copy(
                codes[a].at[q, at], gots[a].at[me, at],
                send_sem.at[m], recv_sem.at[m, me], device_id={"shard": q}, device_id_type=MESH,
            )

        def piece_from(m, s):
            a, first, size = pieces[m]
            ref = gots[a].at[s, pl.ds(first, size)]
            return pltpu.make_async_remote_copy(
                ref, ref, send_sem.at[m], recv_sem.at[m, s], device_id={"shard": s}, device_id_type=MESH
            )

        def all_pieces(m):
            a, _, size = pieces[m]
            ref = codes[a].at[pl.ds(0, n - 1), pl.ds(0, size)]
            return pltpu.make_async_remote_copy(
                ref, ref, send_sem.at[m], recv_sem.at[m, 0], device_id={"shard": me}, device_id_type=MESH
            )

        def own(a):
            return pltpu.make_async_copy(codes[a].at[me], gots[a].at[me], own_sem.at[a])

        def send(m):
            for q in peers:
                piece_to(m, q).start()

        for a in range(3):
            for t in range(2):
                load(a, t).wait()
            produce(a)
            if a == 0:
                pl.semaphore_wait(barrier, n - 1 + n_z - 1)
                send(0)
        attach_sums()
        for m in range(1, len(pieces)):
            send(m)
        for a in range(3):
            own(a).start()

        for a in range(3):
            own(a).wait()
        for q in peers:
            piece_from(1, q).wait_recv()

        def join(c, z):
            whole = jnp.zeros((2 * SUBS, LANES), jnp.float32)
            for k in range(2):
                for h in range(2):
                    v = got_b[2 * c + k, pl.ds(cols * few + h * tile, tile), :].astype(jnp.float32)
                    for side in range(2):
                        to = k * half_lane + (2 * h + side) * quarter
                        moved = pltpu.roll(v, (to - side * half_lane - cols) % LANES, axis=1)
                        whole = jnp.where(jnp.logical_and(lane2 >= to, lane2 < to + quarter), moved, whole)
            zbuf[:, pl.ds(pl.multiple_of(c * LANES, LANES), LANES)] = whole.astype(jnp.bfloat16)
            return z

        lax.fori_loop(0, chips, join, 0)

        def across(d, slot):
            z = lax.rem(plane + d, n_z)
            return pltpu.make_async_remote_copy(
                zbuf, zgot.at[slot], zsend.at[d], zrecv.at[slot], device_id={"expert": z}, device_id_type=MESH
            )

        for d in range(1, n_z):
            across(d, plane).start()
        orr[pl.ds(pl.multiple_of(plane * experts, experts), experts), :] = zbuf[...]

        def factors(h):
            total = lax.fori_loop(0, n, lambda s, t: t + partial(h, s), jnp.zeros((SUBS, LANES), jnp.float32))
            scale = jnp.sqrt(total)
            osg[pl.ds(h * SUBS, SUBS), :] = scale[:, :cols]
            osu[pl.ds(h * SUBS, SUBS), :] = across_lanes(scale)[:, :cols]
            each = 1.0 / (SPAN * scale)
            some = jnp.logical_and(used, total > 0)

            def one(c, z):
                a = jnp.where(some, jnp.sqrt(partial(h, 2 * c)) * each, 0.0)
                b = jnp.where(some, jnp.sqrt(partial(h, 2 * c + 1)) * each, 0.0)
                turned = across_lanes(jnp.where(left, b, a))
                for t, f in ((0, jnp.where(left, a, turned)), (1, jnp.where(left, turned, b))):
                    at = pl.ds(pl.multiple_of(t * chips * SUBS + c * SUBS, SUBS), SUBS)
                    high = f.astype(jnp.bfloat16).astype(jnp.float32)
                    share[at, pl.ds(0, LANES)] = high
                    share[at, pl.ds(LANES, LANES)] = f - high
                return z

            lax.fori_loop(0, chips, one, 0)
            lhs = share[...].astype(jnp.bfloat16)
            k = lax.rem(lax.broadcasted_iota(jnp.int32, (2 * LANES, 2 * LANES), 0), LANES)
            m = lax.broadcasted_iota(jnp.int32, (2 * LANES, 2 * LANES), 1)
            source = k - m // LANES - lax.rem(m, LANES) // half_lane * half_lane

            def two(p, z):
                pick = jnp.where(source == 2 * p, 1.0, 0.0).astype(jnp.bfloat16)
                wide = jnp.dot(lhs, pick, preferred_element_type=jnp.float32)
                spread[h, 2 * p] = wide[:, :LANES]
                spread[h, 2 * p + 1] = wide[:, LANES:]
                return z

            lax.fori_loop(0, cols // 2, two, 0)

        def exponents(v):
            v = v.astype(jnp.float32)
            x = jnp.log2(jnp.abs(v)) + FLOOR
            return jnp.where(v < 0, -x, x)

        def merged(one, two):
            turned = across_lanes(jnp.where(left2, two, one))
            return jnp.where(left2, one, turned), jnp.where(left2, turned, two)

        def decode(m, first, count):
            h = pieces[m][0] // 2

            def chip(i, z):
                dc = lax.rem(START // 2 + MIX * i, chips)
                y = lax.rem(my_y - dc // n_x + n_y, n_y)
                x = lax.rem(my_x - dc % n_x + n_x, n_x)
                at = y * n_x + x
                for k in range(2):
                    @pl.when(2 * at + k != me)
                    def arrival():
                        piece_from(m, 2 * at + k).wait_recv()

                lanes_out = pl.ds(pl.multiple_of(at * LANES, LANES), LANES)

                def put(t, j, x):
                    f = spread[h, j, pl.ds(pl.multiple_of(t * chips * SUBS + at * SUBS, SUBS), SUBS), :]
                    (og, ou)[t][j, pl.ds(h * SUBS, SUBS), lanes_out] = (x * f).astype(jnp.bfloat16)

                if h:
                    for j in range(first, first + count, 2):
                        sides = merged(*(exponents(got_c[2 * at + k, pl.ds(j * SUBS, 2 * SUBS), :]) for k in range(2)))
                        for t in range(2):
                            for r in range(2):
                                put(t, j + r, sides[t][r * SUBS:(r + 1) * SUBS])
                else:
                    for j in range(first, first + count, 4):
                        rng = pl.ds(j * few, 2 * SUBS)
                        one = merged(*(exponents(got_a[2 * at + k, rng, :]) for k in range(2)))
                        two = merged(*(exponents(got_b[2 * at + k, rng, :]) for k in range(2)))
                        for t in range(2):
                            for r in range(2):
                                a, b = one[t][r * SUBS:(r + 1) * SUBS], two[t][r * SUBS:(r + 1) * SUBS]
                                turned = pltpu.roll(jnp.where(upper, b, a), few, axis=0)
                                put(t, j + 2 * r, jnp.where(upper, a, turned))
                                put(t, j + 2 * r + 1, jnp.where(upper, turned, b))
                return z

            lax.fori_loop(0, chips, chip, 0)

        factors(0)
        decode(0, 0, cols)
        factors(1)
        for d in range(1, n_z):
            z = lax.rem(plane + d, n_z)
            across(d, plane).wait_send()
            across(d, z).wait_recv()
            orr[pl.ds(pl.multiple_of(z * experts, experts), experts), :] = zgot[z]
        for i in range(len(PARTS)):
            decode(2 + i, sum(PARTS[:i]), PARTS[i])
        for m in range(len(pieces)):
            all_pieces(m).wait_send()

    return kernel


def in_hbm(array):
    return pltpu.with_memory_space_constraint(array, pltpu.HBM)


def put_out(*refs):
    n = len(refs) // 2
    sems = refs[-1]
    copies = [pltpu.make_async_copy(refs[i], refs[n + i], sems.at[i]) for i in range(n)]
    for c in copies:
        c.start()
    for c in copies:
        c.wait()


def solution(mesh):
    n_z, n = mesh.shape["expert"], mesh.shape["shard"]
    n_y = n_x = 4

    def local(master_gate, master_up, router_weight, router_gain):
        experts, rows, width = master_gate.shape
        cols = width // n
        depth = rows * n
        few = SUBS // 2
        sent = 2 + len(PARTS)
        f32, bf16 = jnp.float32, jnp.bfloat16
        vmem = pl.BlockSpec(memory_space=pltpu.VMEM)
        hbm = pl.BlockSpec(memory_space=pltpu.HBM)
        dma = pltpu.SemaphoreType.DMA
        shapes = (
            jax.ShapeDtypeStruct((cols, experts, depth), bf16),
            jax.ShapeDtypeStruct((cols, experts, depth), bf16),
            jax.ShapeDtypeStruct((experts, cols), f32),
            jax.ShapeDtypeStruct((experts, cols), f32),
            jax.ShapeDtypeStruct((experts * n_z, depth), bf16),
        )
        results = pl.pallas_call(
            make_kernel(experts, rows, width, cols, n_y, n_x, n_z),
            out_shape=shapes,
            in_specs=[hbm] * 4,
            out_specs=(vmem,) * 5,
            scratch_shapes=[
                pltpu.VMEM((experts, rows, width), f32),
                pltpu.VMEM((experts, rows, width), f32),
                pltpu.VMEM((width * SUBS + SUBS, LANES), f32),
                *[pltpu.VMEM((n, r, LANES), bf16) for r in (cols * few, cols * few + 4 * SUBS, cols * SUBS)] * 2,
                pltpu.VMEM((2, 2, SUBS, width + LANES), f32),
                pltpu.VMEM((n * SUBS, 2 * LANES), f32),
                pltpu.VMEM((2, cols, n * SUBS, LANES), f32),
                pltpu.VMEM((experts, rows), f32),
                pltpu.VMEM((1, rows), f32),
                pltpu.VMEM((experts, depth), bf16),
                pltpu.VMEM((n_z, experts, depth), bf16),
                dma((3, 2)), dma((2,)), dma((3,)), dma((sent,)), dma((sent, n)),
                dma((n_z,)), dma((n_z,)),
            ],
            compiler_params=pltpu.CompilerParams(
                collective_id=0, has_side_effects=True, vmem_limit_bytes=45 * 2**20
            ),
        )(master_gate, master_up, in_hbm(router_weight.T), in_hbm(router_gain[None, :]))
        og, ou, osg, osu, orr = pl.pallas_call(
            put_out,
            out_shape=shapes,
            in_specs=[pl.BlockSpec(memory_space=pl.ANY)] * 5,
            out_specs=(hbm,) * 5,
            scratch_shapes=[dma((5,))],
            compiler_params=pltpu.CompilerParams(vmem_limit_bytes=2**20),
        )(*results)
        return og.transpose(1, 2, 0), ou.transpose(1, 2, 0), osg, osu, orr.T

    in_specs = (P("expert", "shard", None), P("expert", "shard", None), P("shard", "expert"), P("shard"))
    out_specs = (P("expert", None, "shard"), P("expert", None, "shard"), P("expert", "shard"), P("expert", "shard"), P())
    return jax.shard_map(local, mesh=mesh, in_specs=in_specs, out_specs=out_specs, check_vma=False)
```

```python
import jax
import jax.numpy as jnp
from jax import lax
from jax.experimental import pallas as pl
from jax.experimental.pallas import tpu as pltpu
from jax.sharding import PartitionSpec as P

MESH = pl.DeviceIdType.MESH
LANES = 128
SUBS = 8
SPAN = 250.0
FLOOR = 124.0
MIX, START = 23, 8
PARTS = (22, 22)


def encoded(x, partial):
    rate = jnp.where(partial > 0, SPAN * lax.rsqrt(partial), 0.0)
    code = jnp.exp2(jnp.abs(x) * rate - FLOOR)
    return jnp.where(x < 0, -code, code)


def make_kernel(experts, rows, width, cols, n_y, n_x, n_z):
    n = n_y * n_x * 2
    chips = n // 2
    few = SUBS // 2
    blocks = width // LANES
    half_lane = LANES // 2
    tile = 2 * SUBS
    pieces = [(0, 0, cols * few), (1, 0, cols * few + 2 * tile)]
    for i in range(len(PARTS)):
        pieces.append((2, sum(PARTS[:i]) * SUBS, PARTS[i] * SUBS))

    def kernel(gate, up, router, gain, og, ou, osg, osu, orr,
               xg, xu, stage, code_a, code_b, code_c, got_a, got_b, got_c, sums, share, spread,
               xr, xgain, zbuf, zgot,
               in_sem, small_sem, own_sem, send_sem, recv_sem, zsend, zrecv):
        codes, gots = (code_a, code_b, code_c), (got_a, got_b, got_c)
        me = lax.axis_index("shard")
        plane = lax.axis_index("expert")
        my_chip, my_k = me // 2, me % 2
        my_y, my_x = my_chip // n_x, my_chip % n_x
        stretches = ((0, few), (few, few), (2 * few, SUBS))

        def load(a, t):
            src, dst = ((gate, xg), (up, xu))[t]
            at = pl.ds(*stretches[a])
            return pltpu.make_async_copy(src.at[at], dst.at[at], in_sem.at[a, t])

        small = [pltpu.make_async_copy(router, xr, small_sem.at[0]), pltpu.make_async_copy(gain, xgain, small_sem.at[1])]
        def chip_at(d):
            y = lax.rem(my_y + d // (2 * n_x), n_y)
            x = lax.rem(my_x + (d // 2) % n_x, n_x)
            return y * n_x + x

        def hops(d):
            y, x = d // (2 * n_x), (d // 2) % n_x
            return min(y, n_y - y) + min(x, n_x - x)

        order = [d for d in ((i * MIX + START) % n for i in range(n)) if d]
        peers = [chip_at(d) * 2 + lax.rem(my_k + d % 2, 2) for d in order]
        barrier = pltpu.get_barrier_semaphore()
        for far in range(n_y // 2 + n_x // 2, -1, -1):
            for d, q in zip(order, peers):
                if hops(d) == far:
                    pl.semaphore_signal(barrier, 1, device_id={"shard": q}, device_id_type=MESH)
            if far == 4:
                for t in range(2):
                    load(0, t).start()
        for d in range(1, n_z):
            pl.semaphore_signal(barrier, 1, device_id={"expert": lax.rem(plane + d, n_z)}, device_id_type=MESH)
        for c in small:
            c.start()
        for a in range(1, 3):
            for t in range(2):
                load(a, t).start()

        row = lax.broadcasted_iota(jnp.int32, (SUBS, LANES), 0)
        lane = lax.broadcasted_iota(jnp.int32, (SUBS, LANES), 1)
        left = lane < half_lane
        left2 = lax.broadcasted_iota(jnp.int32, (2 * SUBS, LANES), 1) < half_lane
        upper = row < few
        lane2 = lax.broadcasted_iota(jnp.int32, (2 * SUBS, LANES), 1)
        used, used2 = lax.rem(lane, half_lane) < cols, lax.rem(lane2, half_lane) < cols
        quarter = half_lane // 4

        def across_lanes(v):
            return pltpu.roll(v, half_lane, axis=1)

        def produce(a):
            first, count = stretches[a]
            h, e0 = first // SUBS, first % SUBS
            size = LANES * count

            def block(b, z):
                at = pl.ds(pl.multiple_of(b * LANES, LANES), LANES)
                for e in range(count):
                    g = xg[first + e, :, at]
                    u = xu[first + e, :, at]
                    pg = jnp.sum(g * g, axis=0, keepdims=True)
                    pu = jnp.sum(u * u, axis=0, keepdims=True)
                    sums[h, 0, pl.ds(e0 + e, 1), at] = pg
                    sums[h, 1, pl.ds(e0 + e, 1), at] = pu
                    both = jnp.concatenate([encoded(g, pg), encoded(u, pu)], axis=0)
                    stage[pl.ds(pl.multiple_of(b * size, size) + e, LANES, stride=count), :] = both.T
                return z

            lax.fori_loop(0, blocks, block, 0)
            own_rows = cols * count

            def pack(q, z):
                rows_q = stage[pl.ds(pl.multiple_of(q * own_rows, 16), own_rows), :]
                codes[a][q, pl.ds(0, own_rows), :] = rows_q.astype(jnp.bfloat16)
                return z

            lax.fori_loop(0, n, pack, 0)

        def attach_sums():
            for c in small:
                c.wait()
            folded = xr[...] * xgain[...]
            folded = jnp.concatenate([folded, folded], axis=1)
            riders = []
            for h in range(2):
                near, far = (pltpu.roll(folded, at - i * quarter, axis=1) for at, i in ((cols, 2 * h), (half_lane + cols, 2 * h + 1)))
                riders.append(jnp.where(left2, near, far))

            def one(q, z):
                first = q * cols
                lo = pl.multiple_of(first // LANES * LANES, LANES)
                s = lax.rem(first, LANES)
                for h in range(2):
                    sides = []
                    for t, shift in ((0, lax.rem(LANES - s, LANES)), (1, lax.rem(LANES + half_lane - s, LANES))):
                        a = pltpu.roll(sums[h, t, :, pl.ds(lo, LANES)], shift, axis=1)
                        b = pltpu.roll(sums[h, t, :, pl.ds(lo + LANES, LANES)], shift, axis=1)
                        sides.append(jnp.where(lane - t * half_lane + s < LANES, a, b))
                    p = jnp.where(left, sides[0], sides[1])
                    high = p.astype(jnp.bfloat16).astype(jnp.float32)
                    parts = jnp.where(used2, jnp.concatenate([high, p - high], axis=0), riders[h])
                    code_b[q, pl.ds(cols * few + h * tile, tile), :] = parts.astype(jnp.bfloat16)
                return z

            lax.fori_loop(0, n, one, 0)

        def partial(h, s):
            parts = got_b[s, pl.ds(cols * few + h * tile, tile), :].astype(jnp.float32)
            return parts[:SUBS] + parts[SUBS:]

        def piece_to(m, q):
            a, first, size = pieces[m]
            at = pl.ds(first, size)
            return pltpu.make_async_remote_copy(
                codes[a].at[q, at], gots[a].at[me, at],
                send_sem.at[m], recv_sem.at[m, me], device_id={"shard": q}, device_id_type=MESH,
            )

        def piece_from(m, s):
            a, first, size = pieces[m]
            ref = gots[a].at[s, pl.ds(first, size)]
            return pltpu.make_async_remote_copy(
                ref, ref, send_sem.at[m], recv_sem.at[m, s], device_id={"shard": s}, device_id_type=MESH
            )

        def all_pieces(m):
            a, _, size = pieces[m]
            ref = codes[a].at[pl.ds(0, n - 1), pl.ds(0, size)]
            return pltpu.make_async_remote_copy(
                ref, ref, send_sem.at[m], recv_sem.at[m, 0], device_id={"shard": me}, device_id_type=MESH
            )

        def own(a):
            return pltpu.make_async_copy(codes[a].at[me], gots[a].at[me], own_sem.at[a])

        def send(m):
            for q in peers:
                piece_to(m, q).start()

        for a in range(3):
            for t in range(2):
                load(a, t).wait()
            produce(a)
            if a == 0:
                pl.semaphore_wait(barrier, n - 1 + n_z - 1)
                send(0)
        attach_sums()
        for m in range(1, len(pieces)):
            send(m)
        for a in range(3):
            own(a).start()

        for a in range(3):
            own(a).wait()
        for q in peers:
            piece_from(1, q).wait_recv()

        def join(c, z):
            whole = jnp.zeros((2 * SUBS, LANES), jnp.float32)
            for k in range(2):
                for h in range(2):
                    v = got_b[2 * c + k, pl.ds(cols * few + h * tile, tile), :].astype(jnp.float32)
                    for side in range(2):
                        to = k * half_lane + (2 * h + side) * quarter
                        moved = pltpu.roll(v, (to - side * half_lane - cols) % LANES, axis=1)
                        whole = jnp.where(jnp.logical_and(lane2 >= to, lane2 < to + quarter), moved, whole)
            zbuf[:, pl.ds(pl.multiple_of(c * LANES, LANES), LANES)] = whole.astype(jnp.bfloat16)
            return z

        lax.fori_loop(0, chips, join, 0)

        def across(d, slot):
            z = lax.rem(plane + d, n_z)
            return pltpu.make_async_remote_copy(
                zbuf, zgot.at[slot], zsend.at[d], zrecv.at[slot], device_id={"expert": z}, device_id_type=MESH
            )

        for d in range(1, n_z):
            across(d, plane).start()
        orr[pl.ds(pl.multiple_of(plane * experts, experts), experts), :] = zbuf[...]

        def factors(h):
            total = lax.fori_loop(0, n, lambda s, t: t + partial(h, s), jnp.zeros((SUBS, LANES), jnp.float32))
            scale = jnp.sqrt(total)
            osg[pl.ds(h * SUBS, SUBS), :] = scale[:, :cols]
            osu[pl.ds(h * SUBS, SUBS), :] = across_lanes(scale)[:, :cols]
            each = 1.0 / (SPAN * scale)
            some = jnp.logical_and(used, total > 0)

            def one(c, z):
                a = jnp.where(some, jnp.sqrt(partial(h, 2 * c)) * each, 0.0)
                b = jnp.where(some, jnp.sqrt(partial(h, 2 * c + 1)) * each, 0.0)
                turned = across_lanes(jnp.where(left, b, a))
                for t, f in ((0, jnp.where(left, a, turned)), (1, jnp.where(left, turned, b))):
                    at = pl.ds(pl.multiple_of(t * chips * SUBS + c * SUBS, SUBS), SUBS)
                    high = f.astype(jnp.bfloat16).astype(jnp.float32)
                    share[at, pl.ds(0, LANES)] = high
                    share[at, pl.ds(LANES, LANES)] = f - high
                return z

            lax.fori_loop(0, chips, one, 0)
            lhs = share[...].astype(jnp.bfloat16)
            k = lax.rem(lax.broadcasted_iota(jnp.int32, (2 * LANES, 2 * LANES), 0), LANES)
            m = lax.broadcasted_iota(jnp.int32, (2 * LANES, 2 * LANES), 1)
            source = k - m // LANES - lax.rem(m, LANES) // half_lane * half_lane

            def two(p, z):
                pick = jnp.where(source == 2 * p, 1.0, 0.0).astype(jnp.bfloat16)
                wide = jnp.dot(lhs, pick, preferred_element_type=jnp.float32)
                spread[h, 2 * p] = wide[:, :LANES]
                spread[h, 2 * p + 1] = wide[:, LANES:]
                return z

            lax.fori_loop(0, cols // 2, two, 0)

        def exponents(v):
            v = v.astype(jnp.float32)
            x = jnp.log2(jnp.abs(v)) + FLOOR
            return jnp.where(v < 0, -x, x)

        def merged(one, two):
            turned = across_lanes(jnp.where(left2, two, one))
            return jnp.where(left2, one, turned), jnp.where(left2, turned, two)

        def decode(m, first, count):
            h = pieces[m][0] // 2

            def chip(i, z):
                dc = lax.rem(START // 2 + MIX * i, chips)
                y = lax.rem(my_y - dc // n_x + n_y, n_y)
                x = lax.rem(my_x - dc % n_x + n_x, n_x)
                at = y * n_x + x
                for k in range(2):
                    @pl.when(2 * at + k != me)
                    def arrival():
                        piece_from(m, 2 * at + k).wait_recv()

                lanes_out = pl.ds(pl.multiple_of(at * LANES, LANES), LANES)

                def put(t, j, x):
                    f = spread[h, j, pl.ds(pl.multiple_of(t * chips * SUBS + at * SUBS, SUBS), SUBS), :]
                    (og, ou)[t][j, pl.ds(h * SUBS, SUBS), lanes_out] = (x * f).astype(jnp.bfloat16)

                if h:
                    for j in range(first, first + count, 2):
                        sides = merged(*(exponents(got_c[2 * at + k, pl.ds(j * SUBS, 2 * SUBS), :]) for k in range(2)))
                        for t in range(2):
                            for r in range(2):
                                put(t, j + r, sides[t][r * SUBS:(r + 1) * SUBS])
                else:
                    for j in range(first, first + count, 4):
                        rng = pl.ds(j * few, 2 * SUBS)
                        one = merged(*(exponents(got_a[2 * at + k, rng, :]) for k in range(2)))
                        two = merged(*(exponents(got_b[2 * at + k, rng, :]) for k in range(2)))
                        for t in range(2):
                            for r in range(2):
                                a, b = one[t][r * SUBS:(r + 1) * SUBS], two[t][r * SUBS:(r + 1) * SUBS]
                                turned = pltpu.roll(jnp.where(upper, b, a), few, axis=0)
                                put(t, j + 2 * r, jnp.where(upper, a, turned))
                                put(t, j + 2 * r + 1, jnp.where(upper, turned, b))
                return z

            lax.fori_loop(0, chips, chip, 0)

        factors(0)
        decode(0, 0, cols)
        factors(1)
        for d in range(1, n_z):
            z = lax.rem(plane + d, n_z)
            across(d, plane).wait_send()
            across(d, z).wait_recv()
            orr[pl.ds(pl.multiple_of(z * experts, experts), experts), :] = zgot[z]
        for i in range(len(PARTS)):
            decode(2 + i, sum(PARTS[:i]), PARTS[i])
        for m in range(len(pieces)):
            all_pieces(m).wait_send()

    return kernel


def in_hbm(array):
    return pltpu.with_memory_space_constraint(array, pltpu.HBM)


def put_out(*refs):
    n = len(refs) // 2
    sems = refs[-1]
    copies = [pltpu.make_async_copy(refs[i], refs[n + i], sems.at[i]) for i in range(n)]
    for c in copies:
        c.start()
    for c in copies:
        c.wait()


def solution(mesh):
    n_z, n = mesh.shape["expert"], mesh.shape["shard"]
    n_y = n_x = 4

    def local(master_gate, master_up, router_weight, router_gain):
        experts, rows, width = master_gate.shape
        cols = width // n
        depth = rows * n
        few = SUBS // 2
        sent = 2 + len(PARTS)
        f32, bf16 = jnp.float32, jnp.bfloat16
        vmem = pl.BlockSpec(memory_space=pltpu.VMEM)
        hbm = pl.BlockSpec(memory_space=pltpu.HBM)
        dma = pltpu.SemaphoreType.DMA
        shapes = (
            jax.ShapeDtypeStruct((cols, experts, depth), bf16),
            jax.ShapeDtypeStruct((cols, experts, depth), bf16),
            jax.ShapeDtypeStruct((experts, cols), f32),
            jax.ShapeDtypeStruct((experts, cols), f32),
            jax.ShapeDtypeStruct((experts * n_z, depth), bf16),
        )
        results = pl.pallas_call(
            make_kernel(experts, rows, width, cols, n_y, n_x, n_z),
            out_shape=shapes,
            in_specs=[hbm] * 4,
            out_specs=(vmem,) * 5,
            scratch_shapes=[
                pltpu.VMEM((experts, rows, width), f32),
                pltpu.VMEM((experts, rows, width), f32),
                pltpu.VMEM((width * SUBS + SUBS, LANES), f32),
                *[pltpu.VMEM((n, r, LANES), bf16) for r in (cols * few, cols * few + 4 * SUBS, cols * SUBS)] * 2,
                pltpu.VMEM((2, 2, SUBS, width + LANES), f32),
                pltpu.VMEM((n * SUBS, 2 * LANES), f32),
                pltpu.VMEM((2, cols, n * SUBS, LANES), f32),
                pltpu.VMEM((experts, rows), f32),
                pltpu.VMEM((1, rows), f32),
                pltpu.VMEM((experts, depth), bf16),
                pltpu.VMEM((n_z, experts, depth), bf16),
                dma((3, 2)), dma((2,)), dma((3,)), dma((sent,)), dma((sent, n)),
                dma((n_z,)), dma((n_z,)),
            ],
            compiler_params=pltpu.CompilerParams(
                collective_id=0, has_side_effects=True, vmem_limit_bytes=45 * 2**20
            ),
        )(master_gate, master_up, in_hbm(router_weight.T), in_hbm(router_gain[None, :]))
        og, ou, osg, osu, orr = pl.pallas_call(
            put_out,
            out_shape=shapes,
            in_specs=[pl.BlockSpec(memory_space=pl.ANY)] * 5,
            out_specs=(hbm,) * 5,
            scratch_shapes=[dma((5,))],
            compiler_params=pltpu.CompilerParams(vmem_limit_bytes=2**20),
        )(*results)
        return og.transpose(1, 2, 0), ou.transpose(1, 2, 0), osg, osu, orr.T

    in_specs = (P("expert", "shard", None), P("expert", "shard", None), P("shard", "expert"), P("shard"))
    out_specs = (P("expert", None, "shard"), P("expert", None, "shard"), P("expert", "shard"), P("expert", "shard"), P())
    return jax.shard_map(local, mesh=mesh, in_specs=in_specs, out_specs=out_specs, check_vma=False)
```
